32 devices in a mesh: dp: 2 (over x), tp: 4 (over z), fsdp: 4 (over y, core).
Axes of the slice: x: 2, y: 2, z: 4, core: 2. Of those that a mesh axis runs over, the one named last changes fastest.
Arguments:
- x: bfloat16 [8, 2048, 2048], P(('dp', 'fsdp')), parts along dimension 0
- w_query: bfloat16 [2, 2048, 2048], P(None, 'fsdp', 'tp')
- w_key: bfloat16 [2, 2048, 2048], P(None, 'fsdp', 'tp')
- w_value: bfloat16 [2, 2048, 2048], P(None, 'fsdp', 'tp')
- w_out: bfloat16 [2, 2048, 2048], P(None, 'tp', 'fsdp')
- w_gate: bfloat16 [2, 2048, 5504], P(None, 'fsdp', 'tp')
- w_up: bfloat16 [2, 2048, 5504], P(None, 'fsdp', 'tp')
- w_down: bfloat16 [2, 5504, 2048], P(None, 'tp', 'fsdp')
- q_norm_w: float32 [2, 2048], P(None, 'tp')
- k_norm_w: float32 [2, 2048], P(None, 'tp')
- attn_norm_w: float32 [2, 2048], P(None, 'fsdp')
- ffn_norm_w: float32 [2, 2048], P(None, 'fsdp')
Outputs:
- output 1: bfloat16 [8, 2048, 2048], P(('dp', 'fsdp')), parts along dimension 0
- output 2: bfloat16 [2, 8, 2048, 16, 128], P(None, ('dp', 'fsdp'), None, 'tp'), parts along dimension 1
- output 3: bfloat16 [2, 8, 2048, 16, 128], P(None, ('dp', 'fsdp'), None, 'tp'), parts along dimension 1
There are 2 independent parts. The reference program is written for one: setup_inputs(seed, part) draws one part's arguments, and reference() takes and returns one part's arrays. A program takes and returns all parts, laid end to end along the dimension named above; an argument that names none is the same for every part.
All inputs are finite; a program needn't handle non-finite values.
Results may differ from the reference program's by a relative error of at most 0.02.
Values are sent between devices in bfloat16 or wider.
A program may use at most 1 GiB of HBM per device.

```python
import jax
import jax.numpy as jnp
from jax import lax

MODEL_DIM = 2048
NUM_HEADS = 16
HEAD_DIM = 128
FF_DIM = 5504
BATCH_SIZE = 4
SEQ_LENGTH = 2048
NUM_LAYERS = 2
NORM_EPS = 1e-6
ROPE_THETA = 500000.0


def setup_inputs(seed: int = 0, part: int = 0) -> dict:
    keys = jax.random.split(jax.random.key(seed), 16)
    part_key = jax.random.fold_in(jax.random.key(seed + 1), part)
    dim_scale = MODEL_DIM ** -0.5
    ff_scale = FF_DIM ** -0.5
    square = (NUM_LAYERS, MODEL_DIM, MODEL_DIM)
    wide = (NUM_LAYERS, MODEL_DIM, FF_DIM)

    def normal_weight(key_w, shape_w, scale_w):
        return (jax.random.normal(key_w, shape_w, jnp.float32) * scale_w).astype(jnp.bfloat16)

    def head_scaled(key_w, key_s):
        weight = jax.random.normal(key_w, (NUM_LAYERS, MODEL_DIM, NUM_HEADS, HEAD_DIM), jnp.float32)
        scales = jnp.exp(jax.random.uniform(key_s, (NUM_LAYERS, 1, NUM_HEADS, 1), jnp.float32, -0.6, 0.6))
        return (weight * scales * dim_scale).reshape(square).astype(jnp.bfloat16)

    def gain(key_g):
        return jax.random.uniform(key_g, (NUM_LAYERS, MODEL_DIM), jnp.float32, 0.5, 1.5)

    x = jax.random.normal(part_key, (BATCH_SIZE, SEQ_LENGTH, MODEL_DIM), jnp.float32)
    return {
        'x': x.astype(jnp.bfloat16),
        'w_query': head_scaled(keys[0], keys[1]),
        'w_key': head_scaled(keys[2], keys[3]),
        'w_value': normal_weight(keys[4], square, dim_scale),
        'w_out': normal_weight(keys[5], square, dim_scale),
        'w_gate': normal_weight(keys[6], wide, dim_scale),
        'w_up': normal_weight(keys[7], wide, dim_scale),
        'w_down': normal_weight(keys[8], (NUM_LAYERS, FF_DIM, MODEL_DIM), ff_scale),
        'q_norm_w': gain(keys[9]),
        'k_norm_w': gain(keys[10]),
        'attn_norm_w': gain(keys[11]),
        'ffn_norm_w': gain(keys[12]),
    }


def rope_tables(seq_len):
    half = HEAD_DIM // 2
    inv_freq = ROPE_THETA ** (-2.0 * jnp.arange(half, dtype=jnp.float32) / HEAD_DIM)
    angles = jnp.arange(seq_len, dtype=jnp.float32)[:, None] * inv_freq[None, :]
    return jnp.cos(angles)[:, None, :], jnp.sin(angles)[:, None, :]


def apply_rope(vals, cos_t, sin_t):
    half = HEAD_DIM // 2
    first = vals[..., :half]
    second = vals[..., half:]
    return jnp.concatenate([first * cos_t - second * sin_t, second * cos_t + first * sin_t], axis=-1)


def rms_scale(vals):
    return lax.rsqrt(jnp.mean(vals * vals, axis=-1, keepdims=True) + NORM_EPS)


def attend_one(operands):
    q_seq, k_seq, v_seq = operands
    seq_len = q_seq.shape[0]
    scores = jnp.einsum('qhd,khd->hqk', q_seq.astype(jnp.float32), k_seq.astype(jnp.float32)) * (HEAD_DIM ** -0.5)
    causal = jnp.arange(seq_len)[:, None] >= jnp.arange(seq_len)[None, :]
    scores = jnp.where(causal[None, :, :], scores, -jnp.inf)
    attn_probs = jax.nn.softmax(scores, axis=-1).astype(jnp.bfloat16)
    result = jnp.einsum('hqk,khd->qhd', attn_probs.astype(jnp.float32), v_seq.astype(jnp.float32))
    return result.astype(jnp.bfloat16)


def layer_step(hidden, weights):
    w_query, w_key, w_value, w_out, w_gate, w_up, w_down, q_gain, k_gain, attn_gain, ffn_gain = weights
    batch, seq_len, width = hidden.shape
    flat = hidden.reshape(batch * seq_len, width)
    head_shape = (batch, seq_len, NUM_HEADS, HEAD_DIM)
    cos_t, sin_t = rope_tables(seq_len)
    q_raw = jnp.dot(flat, w_query, preferred_element_type=jnp.float32)
    k_raw = jnp.dot(flat, w_key, preferred_element_type=jnp.float32)
    values = jnp.dot(flat, w_value, preferred_element_type=jnp.float32).astype(jnp.bfloat16).reshape(head_shape)
    queries = apply_rope((q_raw * rms_scale(q_raw) * q_gain).reshape(head_shape), cos_t, sin_t).astype(jnp.bfloat16)
    keys_rot = apply_rope((k_raw * rms_scale(k_raw) * k_gain).reshape(head_shape), cos_t, sin_t).astype(jnp.bfloat16)
    attended = lax.map(attend_one, (queries, keys_rot, values))
    a_out = jnp.dot(attended.reshape(batch * seq_len, width), w_out, preferred_element_type=jnp.float32)
    a_out = a_out.astype(jnp.bfloat16).astype(jnp.float32)
    h_new = (flat.astype(jnp.float32) + a_out * rms_scale(a_out) * attn_gain).astype(jnp.bfloat16)
    gate = jnp.dot(h_new, w_gate, preferred_element_type=jnp.float32)
    up_val = jnp.dot(h_new, w_up, preferred_element_type=jnp.float32)
    hidden_act = (jax.nn.silu(gate) * up_val).astype(jnp.bfloat16)
    m_out = jnp.dot(hidden_act, w_down, preferred_element_type=jnp.float32)
    m_out = m_out.astype(jnp.bfloat16).astype(jnp.float32)
    result = (h_new.astype(jnp.float32) + m_out * rms_scale(m_out) * ffn_gain).astype(jnp.bfloat16)
    return result.reshape(batch, seq_len, width), (keys_rot, values)


def reference(x, w_query, w_key, w_value, w_out, w_gate, w_up, w_down, q_norm_w, k_norm_w, attn_norm_w, ffn_norm_w):
    stacked = (w_query, w_key, w_value, w_out, w_gate, w_up, w_down, q_norm_w, k_norm_w, attn_norm_w, ffn_norm_w)
    y, caches = lax.scan(layer_step, x, stacked)
    return y, caches[0], caches[1]
```

```python
import functools
import jax
import jax.numpy as jnp
import numpy as np
from jax import lax
from jax.experimental import pallas as pl
from jax.experimental.pallas import tpu as pltpu
from jax.sharding import PartitionSpec as P

HEAD_DIM = 128
NORM_EPS = 1e-6
ROPE_THETA = 500000.0
LOG2E = 1.4426950408889634
MESH = pl.DeviceIdType.MESH
BF16 = jnp.bfloat16
F32 = jnp.float32
N_SEM = 240
D_CUT = 352


def rope_table(seq_len):
    half = HEAD_DIM // 2
    inv_freq = np.float32(ROPE_THETA) ** (-2.0 * np.arange(half, dtype=np.float32) / np.float32(HEAD_DIM))
    angles = np.arange(seq_len, dtype=np.float32)[:, None] * inv_freq.astype(np.float32)[None, :]
    return np.concatenate([np.cos(angles), np.sin(angles)], axis=1).astype(np.float32)


def dot_nt(lhs, rhs):
    return lax.dot_general(lhs, rhs, (((1,), (1,)), ((), ())), preferred_element_type=F32)


def dot_nn(lhs, rhs):
    return jnp.dot(lhs, rhs, preferred_element_type=F32)


def loop(count, body):
    lax.fori_loop(0, count, lambda i, c: (body(i), c)[1], 0)


def mega(x_ref, wq_ref, wk_ref, wv_ref, wo_ref, wg_ref, wu_ref, wd_ref, gain_ref, tab_ref,
         y_ref, kc_ref, vc_ref, aq_ref, ao_ref, ag_ref, au_ref, ad_ref,
         xbuf, hb, ofull, sqb, cosb, sinb, gp, send_sems, recv_sems, loc_sems):
    seq = x_ref.shape[0]
    chunk = seq // 4
    cx, cz, cf = lax.axis_index('dp'), lax.axis_index('tp'), lax.axis_index('fsdp')
    f1 = cf + 1 - 2 * (cf % 2)
    f2 = (cf + 2) % 4
    nx = 1 - cx
    up_z = (cz + 1) % 4
    X = (nx, cz, cf)
    Y = (cx, cz, f2)
    C = (cx, cz, f1)
    Z = (cx, up_z, cf)
    state = {'n': 0}
    sent = []

    def remote(pairs, dev):
        out = []
        for src, dst in pairs:
            n = state['n']
            state['n'] = n + 1
            cp = pltpu.make_async_remote_copy(src_ref=src, dst_ref=dst, send_sem=send_sems.at[n], recv_sem=recv_sems.at[n],
                                              device_id=dev, device_id_type=MESH)
            cp.start()
            out.append((n, frozen(src), frozen(dst)))
        sent.extend(out)
        return out

    def frozen(ref):
        if not getattr(ref, 'transforms', ()):
            return ref, None
        idx, = ref.transforms
        return ref.ref, tuple(int(i.size) if isinstance(i, pl.Slice) else None for i in idx.indices)

    def thawed(item):
        ref, sizes = item
        return ref if sizes is None else ref.at[tuple(0 if s is None else pl.ds(0, s) for s in sizes)]

    def handle(n, src, dst):
        return pltpu.make_async_remote_copy(src_ref=thawed(src), dst_ref=thawed(dst), send_sem=send_sems.at[n], recv_sem=recv_sems.at[n],
                                            device_id=(0, 0, 0), device_id_type=MESH)

    def arrive(cps):
        for cp in cps:
            handle(*cp).wait_recv()

    def flush(cp):
        handle(*cp).wait_send()

    def rows(base, size):
        return pl.ds(base if isinstance(base, int) else pl.multiple_of(base, 16), size)

    class Group:
        def __init__(self, kind, layer):
            self.kind, self.layer, self.tx = kind, layer, {}

        def whole(self, p, f):
            l = self.layer
            if self.kind == 'q':
                return [aq_ref.at[l, i, rows(f * 512, 512), :] for i in range(3)]
            if self.kind == 'o':
                return [ao_ref.at[l, p, f]]
            return [ag_ref.at[l, p, rows(f * 512, 512), :], au_ref.at[l, p, rows(f * 512, 512), :], ad_ref.at[l, p, f]]

        def half(self, p, f, xh):
            l = self.layer
            if self.kind == 'q':
                return [aq_ref.at[l, i, rows(f * 512 + xh * 256, 256), :] for i in range(3)]
            if self.kind == 'o':
                return [ao_ref.at[l, p, f, rows(xh * 256, 256), :]]
            r = rows(f * 512 + xh * 256, 256)
            return [ag_ref.at[l, p, r, :], au_ref.at[l, p, r, :], ad_ref.at[l, p, f, rows(xh * 688, 688), :]]

        def via_x(self, p, f, xh):
            l = self.layer
            if self.kind == 'o':
                return [ao_ref.at[l, p, f, rows(xh * 256, 128), :]]
            return [ag_ref.at[l, p, rows(f * 512 + xh * 256, 256), :], ad_ref.at[l, p, f, rows(xh * 688, D_CUT), :]]

        def via_y(self, p, f, xh):
            l = self.layer
            if self.kind == 'o':
                return [ao_ref.at[l, p, f, rows(xh * 256 + 128, 128), :]]
            return [au_ref.at[l, p, rows(f * 512 + xh * 256, 256), :],
                    ad_ref.at[l, p, f, rows(xh * 688 + D_CUT, 688 - D_CUT), :]]

        def own_whole(self):
            l = self.layer
            if self.kind == 'q':
                return [r.at[l] for r in (wq_ref, wk_ref, wv_ref)]
            if self.kind == 'o':
                return [wo_ref.at[l]]
            return [wg_ref.at[l], wu_ref.at[l], wd_ref.at[l]]

        def own_half(self):
            l = self.layer
            if self.kind == 'q':
                return [r.at[l, rows(cx * 256, 256), :] for r in (wq_ref, wk_ref, wv_ref)]
            if self.kind == 'o':
                return [wo_ref.at[l, rows(cx * 256, 256), :]]
            return [wg_ref.at[l, rows(cx * 256, 256), :], wu_ref.at[l, rows(cx * 256, 256), :],
                    wd_ref.at[l, rows(cx * 688, 688), :]]

        def plane(self, k):
            return (cz + 4 - k) % 4

        def begin_plane(self):
            self.tx['y0'] = remote(zip(self.own_half(), self.half(cz, cf, cx)), Y)
            self.tx['c0'] = remote(zip(self.own_whole(), self.whole(cz, cf)), C)

        def begin_ring(self):
            self.tx['z1'] = remote(zip(self.own_half(), self.half(cz, cf, cx)), Z)

        def got_y0(self):
            arrive(self.tx['y0'])
            refs = self.half(cz, f2, cx)
            self.tx['rx0'] = remote(zip(refs, refs), X)

        def got_rx0(self):
            arrive(self.tx['rx0'])
            refs = self.whole(cz, f2)
            self.tx['d0'] = remote(zip(refs, refs), C)

        def got_z(self, k):
            arrive(self.tx[f'z{k}'])
            refs = self.half(self.plane(k), cf, cx)
            if k < 3:
                self.tx[f'z{k + 1}'] = remote(zip(refs, refs), Z)
            self.tx[f'x{k}'] = remote(zip(refs, refs), X)
            self.tx[f'y{k}'] = remote(zip(refs, refs), Y)

        def got_x(self, k):
            arrive(self.tx[f'x{k}'])
            p = self.plane(k)
            refs = self.via_y(p, cf, nx)
            self.tx[f'ry{k}'] = remote(zip(refs, refs), Y)
            refs = self.whole(p, cf)
            self.tx[f'c{k}'] = remote(zip(refs, refs), C)

        def got_y(self, k):
            arrive(self.tx[f'y{k}'])
            refs = self.via_x(self.plane(k), f2, cx)
            self.tx[f'rx{k}'] = remote(zip(refs, refs), X)

        def got_r(self, k):
            arrive(self.tx[f'rx{k}'])
            arrive(self.tx[f'ry{k}'])
            refs = self.whole(self.plane(k), f2)
            self.tx[f'd{k}'] = remote(zip(refs, refs), C)

        def done(self, k):
            arrive(self.tx[f'c{k}'])
            arrive(self.tx[f'd{k}'])

    def local(src, dst, n):
        cp = pltpu.make_async_copy(src, dst, loc_sems.at[n])
        cp.start()
        return cp

    grp = {(kind, l): Group(kind, l) for kind in 'qom' for l in range(2)}
    q0, o0, m0, q1, o1, m1 = [grp[k] for k in (('q', 0), ('o', 0), ('m', 0), ('q', 1), ('o', 1), ('m', 1))]

    q0.begin_plane()
    o0.begin_ring()
    o0.begin_plane()
    gain_tx = []
    for off in range(1, 4):
        gain_tx.append(remote([(gain_ref, gp.at[cf])], (cx, cz, (cf + off) % 4)))
    ld_x = local(x_ref, xbuf, 0)
    ld_g = local(gain_ref, gp.at[cf], 1)
    ld_t = local(tab_ref, cosb, 2)
    ld_h = local(x_ref.at[rows(cz * chunk, chunk), :], hb, 3)
    ld_t.wait()

    def make_tables(i):
        r = rows(i * 256, 256)
        tab = cosb[r, :]
        rolled = pltpu.roll(tab, 64, 1)
        low = lax.broadcasted_iota(jnp.int32, (256, 128), 1) < 64
        cosb[r, :] = jnp.where(low, tab, rolled)
        sinb[r, :] = jnp.where(low, -rolled, tab)

    loop(seq // 256, make_tables)

    o0.got_z(1)
    o0.got_z(2)
    q0.got_y0()
    o0.got_z(3)
    m0.begin_ring()
    m0.begin_plane()
    o0.got_y0()
    q0.got_rx0()
    for tx in gain_tx:
        arrive(tx)
    q0.done(0)
    ld_x.wait()
    ld_g.wait()
    ld_h.wait()

    def gain_row(i):
        return jnp.concatenate([gp[f, i:i + 1, :] for f in range(4)], axis=1)

    def front(layer, wqkv, raw, qkv, obuf, ag_tx, ticks):
        loads = [local(aq_ref.at[layer, i, rows(((cf + j) % 4) * 512, 512), :],
                       wqkv.at[i, rows(((cf + j) % 4) * 512, 512), :], 4 + i * 4 + j) for i in range(3) for j in range(1, 4)]
        loads += [local(r.at[layer], wqkv.at[i, rows(cf * 512, 512), :], 4 + i * 4)
                  for i, r in enumerate((wq_ref, wk_ref, wv_ref))]
        for cp in loads:
            cp.wait()
        lane = lax.broadcasted_iota(jnp.int32, (256, 128), 1)

        def project(t):
            r = rows(t * 256, 256)
            xt = xbuf[r, :]
            qv = dot_nn(xt, wqkv[0])
            raw[0, r, :] = qv
            kv = dot_nn(xt, wqkv[1])
            raw[1, r, :] = kv
            qkv[2, r, :] = dot_nn(xt, wqkv[2]).astype(BF16)
            qs = jnp.sum(qv * qv, axis=-1, keepdims=True)
            ks = jnp.sum(kv * kv, axis=-1, keepdims=True)
            both = jnp.where(lane == 0, qs, jnp.where(lane == 1, ks, 0.0))
            sqb[layer, cz, :, pl.ds(pl.multiple_of(t * 256, 256), 256)] = both.T[0:8, :]

        if ag_tx is None:
            loop(seq // 256, project)
        else:
            for s in range(4):
                ag_tx(s)
                base = ((cz + 4 - s) % 4) * 2
                loop(2, lambda t: project(base + t))
        sq_tx = []
        for off in range(1, 4):
            ref = sqb.at[layer, cz]
            sq_tx.append(remote([(ref, ref)], (cx, (cz + off) % 4, cf)))
        cp_v = local(qkv.at[2], vc_ref.at[layer], 20)
        ticks[0]()
        for tx in sq_tx:
            arrive(tx)

        def rope(t):
            r = rows(t * 256, 256)
            c = pl.ds(pl.multiple_of(t * 256, 256), 256)
            tot = sqb[layer, 0, :, c] + sqb[layer, 1, :, c] + sqb[layer, 2, :, c] + sqb[layer, 3, :, c]
            inv = lax.rsqrt(tot * (1.0 / (4 * 512)) + NORM_EPS)
            cols = jnp.concatenate([inv] * 16, axis=0).T
            cos_t, sin_t = cosb[r, :], sinb[r, :]
            for i in range(2):
                scale = cols[:, i:i + 1]
                for h in range(4):
                    hs = slice(h * 128, (h + 1) * 128)
                    val = raw[i, r, hs] * scale * gp[cf, 4 + 2 * i + layer:5 + 2 * i + layer, hs]
                    qkv[i, r, hs] = (val * cos_t + pltpu.roll(val, 64, 1) * sin_t).astype(BF16)

        loop(seq // 256, rope)
        cp_k = local(qkv.at[1], kc_ref.at[layer], 21)
        ticks[1]()
        order = (2, 1, 3, 0)
        bq = 256
        sm = (HEAD_DIM ** -0.5) * LOG2E
        o_tx = []

        def attend(off):
            j = (cz + off) % 4

            def step(it):
                h, sub = it // 2, it % 2
                i = 2 * j + sub
                hc = pl.ds(pl.multiple_of(h * 128, 128), 128)
                for n in range(seq // bq):
                    @pl.when(i == n)
                    def _():
                        q_blk = qkv[0, n * bq:(n + 1) * bq, hc]
                        diag = dot_nt(q_blk, qkv[1, n * bq:(n + 1) * bq, hc])
                        ri = lax.broadcasted_iota(jnp.int32, (bq, bq), 0)
                        ci = lax.broadcasted_iota(jnp.int32, (bq, bq), 1)
                        diag = jnp.where(ri >= ci, diag, -jnp.inf)
                        top = jnp.max(diag, axis=-1, keepdims=True)
                        if n:
                            full = dot_nt(q_blk, qkv[1, 0:n * bq, hc])
                            top = jnp.maximum(top, jnp.max(full, axis=-1, keepdims=True))
                        e_diag = jnp.exp2((diag - top) * sm)
                        total = jnp.sum(e_diag, axis=-1, keepdims=True)
                        if n:
                            e_full = jnp.exp2((full - top) * sm)
                            total = total + jnp.sum(e_full, axis=-1, keepdims=True)
                        inv = 1.0 / total
                        out = dot_nn((e_diag * inv).astype(BF16), qkv[2, n * bq:(n + 1) * bq, hc])
                        if n:
                            out = out + dot_nn((e_full * inv).astype(BF16), qkv[2, 0:n * bq, hc])
                        obuf[n * bq:(n + 1) * bq, hc] = out.astype(BF16)

            loop(8, step)

        def attend_all(g):
            off = jnp.where(g == 0, 2, jnp.where(g == 1, 1, jnp.where(g == 2, 3, 0)))
            attend(off)
            for gi, o in enumerate(order[:3]):
                @pl.when(g == gi)
                def _():
                    o_tx[gi].start()

        for o in order[:3]:
            n = state['n']
            state['n'] = n + 1
            j = (cz + o) % 4
            cp = pltpu.make_async_remote_copy(
                src_ref=obuf.at[rows(j * chunk, chunk), :],
                dst_ref=ofull.at[layer, :, pl.ds(pl.multiple_of(cz * 512, 512), 512)],
                send_sem=send_sems.at[n], recv_sem=recv_sems.at[n], device_id=(cx, j, cf), device_id_type=MESH)
            o_tx.append(cp)
        loop(4, attend_all)
        ofull[layer, :, pl.ds(pl.multiple_of(cz * 512, 512), 512)] = obuf[rows(cz * chunk, chunk), :]
        ticks[2]()
        cp_v.wait()
        cp_k.wait()
        for cp in o_tx:
            cp.wait_send()
            cp.wait_recv()

    def proj(layer, wo):
        loads = []
        for p in range(4):
            for f in range(4):
                n = 4 + p * 4 + f
                mine = jnp.logical_and(cz == p, cf == f)

                @pl.when(mine)
                def _():
                    local(wo_ref.at[layer], wo.at[p, f], n)

                @pl.when(jnp.logical_not(mine))
                def _():
                    local(ao_ref.at[layer, p, f], wo.at[p, f], n)
                loads.append(pltpu.make_async_copy(wo_ref.at[layer], wo.at[p, f], loc_sems.at[n]))
        for cp in loads:
            cp.wait()
        gain = gain_row(layer)

        def tile(t):
            r = rows(t * 256, 256)
            ot = ofull[layer, r, :]
            parts = []
            for f in range(4):
                acc = dot_nn(ot[:, 0:512], wo[0, f])
                for p in range(1, 4):
                    acc = acc + dot_nn(ot[:, p * 512:(p + 1) * 512], wo[p, f])
                parts.append(acc.astype(BF16).astype(F32))
            a = jnp.concatenate(parts, axis=1)
            scale = lax.rsqrt(jnp.mean(a * a, axis=-1, keepdims=True) + NORM_EPS)
            hb[r, :] = (hb[r, :].astype(F32) + a * scale * gain).astype(BF16)

        loop(2, tile)

    def mlp(layer, gbuf, ubuf, dbuf, acc, ready, after, finish):
        pend = {}

        def fetch(k):
            s = k % 2
            p = grp[('m', layer)].plane(k)
            cps = []
            base = 4 + s * 12
            for j in range(4):
                f = (cf + j) % 4
                r = rows(f * 512, 512)
                own = k == 0 and j == 0
                g_src = wg_ref.at[layer] if own else ag_ref.at[layer, p, r, :]
                u_src = wu_ref.at[layer] if own else au_ref.at[layer, p, r, :]
                d_src = wd_ref.at[layer] if own else ad_ref.at[layer, p, f]
                cps.append(local(g_src, gbuf.at[s, r, :], base + j))
                cps.append(local(u_src, ubuf.at[s, r, :], base + 4 + j))
                cps.append(local(d_src, dbuf.at[s, f], base + 8 + j))
            pend[k] = cps

        ready(0)
        fetch(0)
        for k in range(4):
            if k < 3 and layer == 1:
                ready(k + 1)
                fetch(k + 1)
            for cp in pend[k]:
                cp.wait()
            s = k % 2

            def tile(t):
                r = rows(t * 256, 256)
                ht = hb[r, :]
                gate = dot_nn(ht, gbuf[s])
                up = dot_nn(ht, ubuf[s])
                act = (jax.nn.silu(gate) * up).astype(BF16)
                for f in range(4):
                    c = slice(f * 512, (f + 1) * 512)
                    val = dot_nn(act, dbuf[s, f])
                    if k:
                        val = val + acc[r, c]
                    acc[r, c] = val
                if k == 3:
                    m = acc[r, :].astype(BF16).astype(F32)
                    scale = lax.rsqrt(jnp.mean(m * m, axis=-1, keepdims=True) + NORM_EPS)
                    hb[r, :] = (hb[r, :].astype(F32) + m * scale * gain_row(2 + layer)).astype(BF16)

            if k < 3:
                loop(2, tile)
                after(k)
                if layer == 0:
                    ready(k + 1)
                    fetch(k + 1)
            else:
                for t in range(2):
                    tile(t)
                    finish(t)

    front_scope = dict(wqkv=pltpu.VMEM((3, seq, 512), BF16), raw=pltpu.VMEM((2, seq, 512), F32),
                       qkv=pltpu.VMEM((3, seq, 512), BF16), obuf=pltpu.VMEM((seq, 512), BF16))
    mlp_scope = dict(gbuf=pltpu.VMEM((2, 2048, 1376), BF16), ubuf=pltpu.VMEM((2, 2048, 1376), BF16),
                     dbuf=pltpu.VMEM((2, 4, 1376, 512), BF16), acc=pltpu.VMEM((chunk, 2048), F32))

    def nothing():
        pass

    def tick_a():
        for k in range(1, 4):
            o0.got_x(k)
            o0.got_y(k)
        o0.got_rx0()

    def tick_b():
        m0.got_z(1)
        for k in range(1, 4):
            o0.got_r(k)

    def tick_c():
        m0.got_y0()
        for k in range(4):
            o0.done(k)

    pl.run_scoped(lambda **kw: front(0, ag_tx=None, ticks=(tick_a, tick_b, tick_c), **kw), **front_scope)
    m0.got_z(2)
    pl.run_scoped(lambda wo: proj(0, wo), pltpu.VMEM((4, 4, 512, 512), BF16))
    m0.got_x(1)
    m0.got_y(1)

    def ready0(k):
        if k == 0:
            m0.got_z(3)
            m0.got_rx0()
            m0.got_x(2)
            m0.got_y(2)
        if k == 1:
            m0.got_r(1)
        if k == 2:
            m0.got_x(3)
            m0.got_y(3)
            q1.begin_plane()
            o1.begin_plane()
            m1.begin_plane()
            m0.got_r(2)
        if k == 3:
            m0.got_r(3)
        m0.done(k)

    def after0(k):
        if k == 0:
            o1.begin_ring()
            m1.begin_ring()
        if k == 1:
            o1.got_z(1)
            o1.got_z(2)

    ag = {}

    def finish0(t):
        blk = rows(cz * chunk + t * 256, 256)
        ag[(0, t)] = remote([(hb.at[rows(t * 256, 256), :], xbuf.at[blk, :])], Z)
        xbuf[blk, :] = hb[rows(t * 256, 256), :]

    pl.run_scoped(lambda **kw: mlp(0, ready=ready0, after=after0, finish=finish0, **kw), **mlp_scope)

    def ag_step(s):
        if s == 0:
            q1.got_y0()
            o1.got_z(3)
            o1.got_y0()
            q1.got_rx0()
            q1.done(0)
            return
        for t in range(2):
            arrive(ag[(s - 1, t)])
            if s < 3:
                blk = rows(((cz + 4 - s) % 4) * chunk + t * 256, 256)
                ag[(s, t)] = remote([(xbuf.at[blk, :], xbuf.at[blk, :])], Z)
        if s == 1:
            m1.got_z(1)
            for k in range(1, 4):
                o1.got_x(k)
                o1.got_y(k)
            o1.got_rx0()
            m1.got_y0()
        if s == 2:
            for k in range(1, 4):
                o1.got_r(k)
            m1.got_x(1)
            m1.got_y(1)
            m1.got_z(2)

    def tick_d():
        m1.got_rx0()

    def tick_f():
        for k in range(4):
            o1.done(k)
        m1.got_r(1)
        m1.got_z(3)

    def front_one(**kw):
        ag_step(0)
        front(1, ag_tx=lambda s: ag_step(s) if s else None, ticks=(tick_d, nothing, tick_f), **kw)

    pl.run_scoped(front_one, **front_scope)
    for s in range(3):
        for t in range(2):
            flush(ag[(s, t)][0])
    pl.run_scoped(lambda wo: proj(1, wo), pltpu.VMEM((4, 4, 512, 512), BF16))

    def ready1(k):
        if k == 0:
            m1.got_x(2)
            m1.got_y(2)
        if k == 2:
            m1.got_x(3)
            m1.got_y(3)
            m1.got_r(2)
        if k == 3:
            m1.got_r(3)
        m1.done(k)

    fin = {}

    def finish1(t):
        blk = rows(cz * chunk + t * 256, 256)
        fin[(0, t)] = remote([(hb.at[rows(t * 256, 256), :], y_ref.at[blk, :])], Z)
        local(hb.at[rows(t * 256, 256), :], y_ref.at[blk, :], 1 + t)

    pl.run_scoped(lambda **kw: mlp(1, ready=ready1, after=lambda k: None, finish=finish1, **kw), **mlp_scope)
    for s in range(1, 4):
        for t in range(2):
            arrive(fin[(s - 1, t)])
            if s < 3:
                blk = rows(((cz + 4 - s) % 4) * chunk + t * 256, 256)
                fin[(s, t)] = remote([(y_ref.at[blk, :], y_ref.at[blk, :])], Z)
    for t in range(2):
        pltpu.make_async_copy(hb.at[rows(t * 256, 256), :], y_ref.at[rows(t * 256, 256), :], loc_sems.at[1 + t]).wait()
    waited = {id(ag[(s, t)][0]) for s in range(3) for t in range(2)}
    for cp in sent:
        if id(cp) not in waited:
            flush(cp)
    assert state['n'] <= N_SEM


def mega_call(x, wq, wk, wv, wo, wg, wu, wd, gains, tab):
    seq, width = x.shape
    any_spec = pl.BlockSpec(memory_space=pl.ANY)
    chunk = seq // 4
    outs = [jax.ShapeDtypeStruct((seq, width), BF16),
            jax.ShapeDtypeStruct((2, seq, 512), BF16), jax.ShapeDtypeStruct((2, seq, 512), BF16),
            jax.ShapeDtypeStruct((2, 3, 2048, 512), BF16), jax.ShapeDtypeStruct((2, 4, 4, 512, 512), BF16),
            jax.ShapeDtypeStruct((2, 4, 2048, 1376), BF16), jax.ShapeDtypeStruct((2, 4, 2048, 1376), BF16),
            jax.ShapeDtypeStruct((2, 4, 4, 1376, 512), BF16)]
    return pl.pallas_call(
        mega,
        in_specs=[any_spec] * 10,
        out_specs=[any_spec] * 8,
        out_shape=outs,
        scratch_shapes=[pltpu.VMEM((seq, width), BF16), pltpu.VMEM((chunk, width), BF16),
                        pltpu.VMEM((2, chunk, width), BF16), pltpu.VMEM((2, 4, 8, seq), F32),
                        pltpu.VMEM((seq, 128), F32), pltpu.VMEM((seq, 128), F32), pltpu.VMEM((4, 8, 512), F32),
                        pltpu.SemaphoreType.DMA((N_SEM,)), pltpu.SemaphoreType.DMA((N_SEM,)),
                        pltpu.SemaphoreType.DMA((32,))],
        compiler_params=pltpu.CompilerParams(has_side_effects=True, vmem_limit_bytes=67043328),
        name='mega')(x, wq, wk, wv, wo, wg, wu, wd, gains, tab)


def solution(mesh):
    batch_axes = ('dp', 'fsdp')
    act_spec = P(batch_axes, None, None)
    in_cols = P(None, 'fsdp', 'tp')
    in_rows = P(None, 'tp', 'fsdp')
    tp_gain = P(None, 'tp')
    fsdp_gain = P(None, 'fsdp')
    cache_spec = P(None, batch_axes, None, 'tp', None)

    def local_layers(x, w_query, w_key, w_value, w_out, w_gate, w_up, w_down, q_norm_w, k_norm_w, attn_norm_w, ffn_norm_w):
        batch, seq_len, width = x.shape
        gains = jnp.concatenate([attn_norm_w, ffn_norm_w, q_norm_w, k_norm_w], axis=0)
        tab = jnp.asarray(rope_table(seq_len))
        outs = mega_call(x.reshape(seq_len, width), w_query, w_key, w_value, w_out, w_gate, w_up, w_down, gains, tab)
        shape = (2, 1, seq_len, 4, HEAD_DIM)
        return outs[0].reshape(x.shape), outs[1].reshape(shape), outs[2].reshape(shape)

    return jax.shard_map(local_layers, mesh=mesh,
                         in_specs=(act_spec, in_cols, in_cols, in_cols, in_rows, in_cols, in_cols, in_rows,
                                   tp_gain, tp_gain, fsdp_gain, fsdp_gain),
                         out_specs=(act_spec, cache_spec, cache_spec), check_vma=False)
```

```python
import functools
import jax
import jax.numpy as jnp
import numpy as np
from jax import lax
from jax.experimental import pallas as pl
from jax.experimental.pallas import tpu as pltpu
from jax.sharding import PartitionSpec as P

HEAD_DIM = 128
NORM_EPS = 1e-6
ROPE_THETA = 500000.0
LOG2E = 1.4426950408889634
MESH = pl.DeviceIdType.MESH
BF16 = jnp.bfloat16
F32 = jnp.float32
N_SEM = 300
TILE = 256
BLK = 512
LANE = 128
F_HALF = 688
S1, S2, S3 = SLOTS = (1, 2, 3)
PAIR = range(2)
TRIO = range(3)
QUAD = range(4)
ALL = slice(None)


def rope_table(seq_len):
    half = HEAD_DIM // 2
    inv_freq = np.float32(ROPE_THETA) ** (-2.0 * np.arange(half, dtype=np.float32) / np.float32(HEAD_DIM))
    angles = np.arange(seq_len, dtype=np.float32)[:, None] * inv_freq.astype(np.float32)[None, :]
    return np.concatenate([np.cos(angles), np.sin(angles)], axis=1).astype(np.float32)


def dot_nt(lhs, rhs):
    return lax.dot_general(lhs, rhs, (((1,), (1,)), ((), ())), preferred_element_type=F32)


def dot_nn(lhs, rhs):
    return jnp.dot(lhs, rhs, preferred_element_type=F32)


def loop(count, body):
    lax.fori_loop(0, count, lambda i, c: (body(i), c)[1], 0)


def mega(x_ref, wq_ref, wk_ref, wv_ref, wo_ref, wg_ref, wu_ref, wd_ref, gain_ref, tab_ref,
         y_ref, kc_ref, vc_ref, aq_ref, ao_ref, aw_ref, bw_ref,
         xbuf, hb, mrecv, ofull, sqb, cosb, sinb, gp, send_sems, recv_sems, loc_sems):
    seq = x_ref.shape[0]
    chunk = seq // 4
    cx, cz, cf = lax.axis_index('dp'), lax.axis_index('tp'), lax.axis_index('fsdp')
    cy = cf // 2
    f1 = cf + 1 - 2 * (cf % 2)
    f2 = (cf + 2) % 4
    nx = 1 - cx
    X = (nx, cz, cf)
    Y = (cx, cz, f2)
    C = (cx, cz, f1)
    mid = (cz + 1) // 2 == 1
    half_z = cz // 2
    outer = 3 * half_z
    state = {'send': 0, 'recv': 0}
    sent = []

    def take_number(kind):
        state[kind] += 1
        return state[kind] - 1

    def frozen(ref):
        if not getattr(ref, 'transforms', ()):
            return ref, None
        idx, = ref.transforms
        return ref.ref, tuple(int(i.size) if isinstance(i, pl.Slice) else None for i in idx.indices)

    def thawed(item):
        ref, sizes = item
        return ref if sizes is None else ref.at[tuple(0 if s is None else pl.ds(0, s) for s in sizes)]

    def expect(pairs):
        return [(take_number('recv'), frozen(dst)) for _, dst in pairs]

    def remote(pairs, dev, into=None, when=None):
        pairs = list(pairs)
        into = expect(pairs) if into is None else into
        for (src, dst), (n, _) in zip(pairs, into):
            m = take_number('send')
            cp = pltpu.make_async_remote_copy(src_ref=src, dst_ref=dst, send_sem=send_sems.at[m], recv_sem=recv_sems.at[n],
                                              device_id=dev, device_id_type=MESH)
            cp.start()
            sent.append((m, frozen(src), when))
        return into

    def handle(ref, m, n):
        return pltpu.make_async_remote_copy(src_ref=thawed(ref), dst_ref=thawed(ref), send_sem=send_sems.at[m],
                                            recv_sem=recv_sems.at[n], device_id=(0, 0, 0), device_id_type=MESH)

    def arrive(cps, name='recv'):
        with jax.named_scope(name):
            for n, ref in cps:
                handle(ref, 0, n).wait_recv()

    def flush(first=0, last=None):
        for m, ref, when in sent[first:last]:
            if m in flushed:
                continue
            flushed.add(m)
            if when is None:
                handle(ref, m, 0).wait_send()
            else:
                @pl.when(mid if when == 'mid' else jnp.logical_not(mid))
                def _():
                    handle(ref, m, 0).wait_send()

    flushed = set()

    def slot_plane(k):
        return (cz, 1 - cz + 4 * half_z, 2 - half_z, 3 - 3 * half_z)[k]

    class Cast:
        def __init__(self, name):
            self.name, self.slots, self.heard = name, None, set()

        def push(self, k, pairs):
            pairs = list(pairs)
            if self.slots is None:
                self.slots = [None] + [expect(pairs) for _ in TRIO]

            @pl.when(mid)
            def _():
                if k < 2:
                    remote(pairs, (cx, 3 - cz, cf), self.slots[2 + k], 'mid')
                if k != 1:
                    remote(pairs, (cx, outer, cf), self.slots[max(k, 1)], 'mid')
            if k == 0:
                @pl.when(jnp.logical_not(mid))
                def _():
                    remote(pairs, (cx, 1 + half_z, cf), self.slots[1], 'end')

        def hear(self, k):
            if k not in self.heard:
                self.heard.add(k)

                @pl.when(mid)
                def _():
                    arrive(self.slots[k], f'relay_{self.name}_{k}')

        def relay(self, k, pairs):
            self.hear(k)
            self.push(k, pairs)

        def take(self, k):
            self.hear(k)

            @pl.when(jnp.logical_not(mid))
            def _():
                arrive(self.slots[k], f'take_{self.name}_{k}')

    def rows(base, size):
        return pl.ds(base if isinstance(base, int) else pl.multiple_of(base, 16), size)

    def cols(base, size):
        return pl.ds(base if isinstance(base, int) else pl.multiple_of(base, LANE), size)

    def same(refs):
        return list(zip(refs, refs))

    class Group:
        def __init__(self, kind, layer):
            self.kind, self.layer, self.tx = kind, layer, {}

        def plane(self, k):
            return slot_plane(k)

        def cast(self, key):
            name = f'{self.kind}{self.layer}{key}'
            return self.tx.setdefault('cast' + key, Cast(name))

        def wait(self, *keys):
            for key in keys:
                arrive(self.tx[key], f'wait_{self.kind}{self.layer}_{key}')

        def send(self, key, pairs, dev):
            self.tx[key] = remote(pairs, dev)

    class QGroup(Group):
        def whole(self, i, f):
            return aq_ref.at[self.layer, i, rows(f * BLK, BLK), :]

        def half(self, i, f):
            return aq_ref.at[self.layer, i, rows(f * BLK + cx * TILE, TILE), :]

        def begin(self):
            own = (wq_ref, wk_ref, wv_ref)
            for i in TRIO:
                self.send(f'y{i}', [(own[i].at[self.layer, rows(cx * TILE, TILE), :], self.half(i, cf))], Y)
            for i in TRIO:
                self.send(f'c{i}', [(own[i].at[self.layer], self.whole(i, cf))], C)

        def got_y(self, i):
            self.wait(f'y{i}')
            self.send(f'r{i}', same([self.half(i, f2)]), X)

        def got_r(self, i):
            self.wait(f'r{i}')
            self.send(f'd{i}', same([self.whole(i, f2)]), C)

        def done(self):
            for i in TRIO:
                self.wait(f'c{i}', f'd{i}')

    class OGroup(Group):
        def whole(self, p, f):
            return ao_ref.at[self.layer, p, f]

        def part(self, p, f, first, size):
            return ao_ref.at[self.layer, p, f, rows(first, size), :]

        def begin(self):
            half = self.part(cz, cf, cx * TILE, TILE)
            src = wo_ref.at[self.layer, rows(cx * TILE, TILE), :]
            self.cast('').push(0, [(src, half)])

        def begin_y(self):
            own, half = wo_ref.at[self.layer], self.part(cz, cf, cx * TILE, TILE)
            src = wo_ref.at[self.layer, rows(cx * TILE, TILE), :]
            self.send('y0', [(src, half)], Y)
            self.send('c0', [(own, self.whole(cz, cf))], C)

        def got_y0(self):
            self.wait('y0')
            self.send('rx0', same([self.part(cz, f2, cx * TILE, TILE)]), X)

        def got_rx0(self):
            self.wait('rx0')
            self.send('d0', same([self.whole(cz, f2)]), C)

        def relay(self, k):
            self.cast('').relay(k, same([self.part(self.plane(k), cf, cx * TILE, TILE)]))

        def take(self, k):
            self.cast('').take(k)
            refs = same([self.part(self.plane(k), cf, cx * TILE, TILE)])
            self.send(f'x{k}', refs, X)
            self.send(f'y{k}', refs, Y)

        def got_xy(self, k):
            p = self.plane(k)
            self.wait(f'x{k}')
            self.send(f'ry{k}', same([self.part(p, cf, nx * TILE + LANE, LANE)]), Y)
            self.send(f'c{k}', same([self.whole(p, cf)]), C)
            self.wait(f'y{k}')
            self.send(f'rx{k}', same([self.part(p, f2, cx * TILE, LANE)]), X)

        def got_r(self, k):
            self.wait(f'rx{k}', f'ry{k}')
            self.send(f'd{k}', same([self.whole(self.plane(k), f2)]), C)

        def done(self):
            for k in QUAD:
                self.wait(f'c{k}', f'd{k}')

    class MGroup(Group):
        def whole(self, p, f):
            return aw_ref.at[p, f]

        def lane(self, p, f, i):
            return aw_ref.at[p, f, i, :, cols(cx * TILE, TILE)]

        def first(self, f, xh, own_y, i):
            src = (wg_ref, wu_ref, wd_ref)[i].at[self.layer, rows(own_y * F_HALF, F_HALF), cols(xh * TILE, TILE)]
            return src, aw_ref.at[cz, f, i, :, cols(xh * TILE, TILE)]

        def begin_ring(self):
            self.cast('a').push(0, [self.first(cf, cx, cy, i) for i in TRIO])

        def begin_y(self):
            self.send('ya', [self.first(cf, cx, 1 - cy, i) for i in TRIO], Y)

        def begin_y_rest(self):
            self.send('yb', [self.first(cf, nx, 1 - cy, i) for i in TRIO], Y)

        def begin_c(self):
            self.send('c0', [((wg_ref, wu_ref, wd_ref)[i].at[self.layer, rows(cy * F_HALF, F_HALF), :], aw_ref.at[cz, cf, i])
                             for i in TRIO], C)

        def got_ya(self):
            self.wait('ya')
            self.cast('b').push(0, same([self.lane(cz, f2, i) for i in TRIO]))

        def got_yb(self):
            self.wait('yb')
            self.send('d0', same([self.whole(cz, f2)]), C)

        def relay(self, ab, k):
            f = cf if ab == 'a' else f2
            self.cast(ab).relay(k, same([self.lane(self.plane(k), f, i) for i in TRIO]))

        def take(self, ab, k):
            self.cast(ab).take(k)
            f = cf if ab == 'a' else f2
            self.send(f'x{ab}{k}', same([self.lane(self.plane(k), f, i) for i in TRIO]), X)

        def got_x(self, ab, k):
            self.wait(f'x{ab}{k}')
            self.send(f"{'c' if ab == 'a' else 'd'}{k}", same([self.whole(self.plane(k), cf if ab == 'a' else f2)]), C)

        def done(self, k):
            self.wait(f'c{k}', f'd{k}')

    class WideGroup(Group):
        def srcs(self):
            return [r.at[self.layer, rows(cx * F_HALF, F_HALF), :] for r in (wg_ref, wu_ref, wd_ref)]

        def block(self, p, f, i):
            return bw_ref.at[p, f, i]

        def half(self, p, f, xh, i):
            return bw_ref.at[p, f, i, rows(xh * F_HALF, F_HALF), :]

        def quarter(self, p, f, xh, i, side):
            return bw_ref.at[p, f, i, rows(xh * F_HALF, F_HALF), pl.ds(side * TILE, TILE)]

        def begin_ring(self, i):
            self.cast(f'{i}').push(0, [(self.srcs()[i], self.half(cz, cf, cx, i))])

        def begin_y(self):
            for i in TRIO:
                self.send(f'y0{i}', [(self.srcs()[i], self.half(cz, cf, cx, i))], Y)

        def begin_c(self):
            own = [r.at[self.layer] for r in (wg_ref, wu_ref, wd_ref)]
            self.send('c0', [(own[i], self.block(cz, cf, i)) for i in TRIO], C)

        def got_y0(self, i):
            self.wait(f'y0{i}')
            self.send(f'r0{i}', same([self.half(cz, f2, cx, i)]), X)

        def got_r0(self):
            self.wait('r00', 'r01', 'r02')
            self.send('d0', same([bw_ref.at[cz, f2]]), C)

        def relay(self, k, i):
            self.cast(f'{i}').relay(k, same([self.half(self.plane(k), cf, cx, i)]))

        def take(self, k, i, spread=True):
            self.cast(f'{i}').take(k)
            self.send(f'x{k}{i}', same([self.half(self.plane(k), cf, cx, i)]), X)
            if spread:
                self.spread(k, i)

        def spread(self, k, i):
            self.send(f'y{k}{i}', same([self.half(self.plane(k), cf, cx, i)]), Y)

        def got_xy(self, k, i):
            p = self.plane(k)
            self.wait(f'x{k}{i}')
            self.send(f'ry{k}{i}', same([self.quarter(p, cf, nx, i, 1)]), Y)
            self.send(f'c{k}{i}', same([self.block(p, cf, i)]), C)
            self.wait(f'y{k}{i}')
            self.send(f'rx{k}{i}', same([self.quarter(p, f2, cx, i, 0)]), X)

        def got_r(self, k, i):
            self.wait(f'rx{k}{i}', f'ry{k}{i}')
            self.send(f'd{k}{i}', same([self.block(self.plane(k), f2, i)]), C)

        def done(self, k):
            if k == 0:
                self.wait('c0', 'd0')
            else:
                for i in TRIO:
                    self.wait(f'c{k}{i}', f'd{k}{i}')

    def local(src, dst, n):
        cp = pltpu.make_async_copy(src, dst, loc_sems.at[n])
        cp.start()
        return cp

    q0, o0, m0 = QGroup('q', 0), OGroup('o', 0), MGroup('m', 0)
    q1, o1, m1 = QGroup('q', 1), OGroup('o', 1), WideGroup('m', 1)

    o0.begin()
    gain_tx = []
    for off in SLOTS:
        gain_tx.append(remote([(gain_ref, gp.at[cf])], (cx, cz, (cf + off) % 4)))
    q0.begin()
    o0.begin_y()
    m0.begin_y()
    m0.begin_c()
    ld_x = local(x_ref, xbuf, 0)
    ld_g = local(gain_ref, gp.at[cf], 1)
    ld_t = local(tab_ref, cosb, 2)
    ld_h = local(x_ref.at[rows(cz * chunk, chunk), :], hb.at[rows(0, chunk), :], 3)
    ld_t.wait()

    def make_tables(i):
        r = rows(i * TILE, TILE)
        tab = cosb[r, :]
        rolled = pltpu.roll(tab, 64, 1)
        low = lax.broadcasted_iota(jnp.int32, (TILE, LANE), 1) < 64
        cosb[r, :] = jnp.where(low, tab, rolled)
        sinb[r, :] = jnp.where(low, -rolled, tab)

    with jax.named_scope('tables'):
        loop(seq // TILE, make_tables)

    o0.relay(1)
    o0.relay(2)
    m0.begin_ring()
    o0.take(1)
    for i in TRIO:
        q0.got_y(i)
    o0.relay(3)
    o0.got_y0()
    for i in TRIO:
        q0.got_r(i)
    for tx in gain_tx:
        arrive(tx)
    q0.done()
    m0.relay('a', 1)
    m0.relay('a', 2)
    ld_x.wait()
    ld_g.wait()
    ld_h.wait()

    def gain_row(i):
        return jnp.concatenate([gp[f, i:i + 1, :] for f in QUAD], axis=1)

    def front(layer, wqkv, raw, qkv, obuf, ag_tx, ticks, mid_hooks):
        loads = [local(aq_ref.at[layer, i, rows(((cf + j) % 4) * BLK, BLK), :],
                       wqkv.at[i, rows(((cf + j) % 4) * BLK, BLK), :], 4 + i * 4 + j) for i in TRIO for j in SLOTS]
        loads += [local(r.at[layer], wqkv.at[i, rows(cf * BLK, BLK), :], 4 + i * 4)
                  for i, r in enumerate((wq_ref, wk_ref, wv_ref))]
        with jax.named_scope('wait_wqkv'):
            for cp in loads:
                cp.wait()
        lane = lax.broadcasted_iota(jnp.int32, (TILE, LANE), 1)

        def project(t):
            r = rows(t * TILE, TILE)
            xt = xbuf[r, :]
            qv = dot_nn(xt, wqkv[0])
            raw[0, r, :] = qv
            kv = dot_nn(xt, wqkv[1])
            raw[1, r, :] = kv
            qkv[2, r, :] = dot_nn(xt, wqkv[2]).astype(BF16)
            qs = jnp.sum(qv * qv, axis=-1, keepdims=True)
            ks = jnp.sum(kv * kv, axis=-1, keepdims=True)
            both = jnp.where(lane == 0, qs, jnp.where(lane == 1, ks, 0.0))
            sqb[layer, cz, :, pl.ds(pl.multiple_of(t * TILE, TILE), TILE)] = both.T[0:8, :]

        if ag_tx is None:
            with jax.named_scope('project'):
                loop(seq // TILE, project)
        else:
            for s in QUAD:
                ag_tx(s)
                base = slot_plane(s) * 2
                with jax.named_scope('project'):
                    loop(2, lambda t: project(base + t))
        sq_tx = []
        for off in SLOTS:
            ref = sqb.at[layer, cz]
            sq_tx.append(remote([(ref, ref)], (cx, (cz + off) % 4, cf)))
        cp_v = local(qkv.at[2], vc_ref.at[layer], 20)
        ticks[0]()
        for tx in sq_tx:
            arrive(tx, 'wait_sq')

        def rope(t):
            r = rows(t * TILE, TILE)
            c = pl.ds(pl.multiple_of(t * TILE, TILE), TILE)
            tot = sqb[layer, 0, :, c] + sqb[layer, 1, :, c] + sqb[layer, 2, :, c] + sqb[layer, 3, :, c]
            inv = lax.rsqrt(tot * (1.0 / (4 * BLK)) + NORM_EPS)
            cols = jnp.concatenate([inv] * 16, axis=0).T
            cos_t, sin_t = cosb[r, :], sinb[r, :]
            for i in PAIR:
                scale = cols[:, i:i + 1]
                for h in QUAD:
                    hs = slice(h * LANE, (h + 1) * LANE)
                    val = raw[i, r, hs] * scale * gp[cf, 4 + 2 * i + layer:5 + 2 * i + layer, hs]
                    qkv[i, r, hs] = (val * cos_t + pltpu.roll(val, 64, 1) * sin_t).astype(BF16)

        with jax.named_scope('rope'):
            loop(seq // TILE, rope)
        cp_k = local(qkv.at[1], kc_ref.at[layer], 21)
        ticks[1]()
        order = (2, 1, 3, 0)
        bq = TILE
        sm = (HEAD_DIM ** -0.5) * LOG2E
        o_tx = []

        def attend(off):
            j = (cz + off) % 4

            def step(it):
                h, sub = it // 2, it % 2
                i = 2 * j + sub
                hc = pl.ds(pl.multiple_of(h * LANE, LANE), LANE)
                for n in range(seq // bq):
                    @pl.when(i == n)
                    def _():
                        q_blk = qkv[0, n * bq:(n + 1) * bq, hc]
                        diag = dot_nt(q_blk, qkv[1, n * bq:(n + 1) * bq, hc])
                        ri = lax.broadcasted_iota(jnp.int32, (bq, bq), 0)
                        ci = lax.broadcasted_iota(jnp.int32, (bq, bq), 1)
                        diag = jnp.where(ri >= ci, diag, -jnp.inf)
                        top = jnp.max(diag, axis=-1, keepdims=True)
                        if n:
                            full = dot_nt(q_blk, qkv[1, 0:n * bq, hc])
                            top = jnp.maximum(top, jnp.max(full, axis=-1, keepdims=True))
                        e_diag = jnp.exp2((diag - top) * sm)
                        total = jnp.sum(e_diag, axis=-1, keepdims=True)
                        if n:
                            e_full = jnp.exp2((full - top) * sm)
                            total = total + jnp.sum(e_full, axis=-1, keepdims=True)
                        inv = 1.0 / total
                        out = dot_nn((e_diag * inv).astype(BF16), qkv[2, n * bq:(n + 1) * bq, hc])
                        if n:
                            out = out + dot_nn((e_full * inv).astype(BF16), qkv[2, 0:n * bq, hc])
                        obuf[n * bq:(n + 1) * bq, hc] = out.astype(BF16)

            loop(8, step)

        def attend_all(g):
            off = jnp.where(g == 0, 2, jnp.where(g == 1, 1, jnp.where(g == 2, 3, 0)))
            attend(off)
            for gi, o in enumerate(order[:3]):
                @pl.when(g == gi)
                def _():
                    o_tx[gi].start()
                    mid_hooks[gi]()

        for o in order[:3]:
            m, n = take_number('send'), take_number('recv')
            j = (cz + o) % 4
            cp = pltpu.make_async_remote_copy(
                src_ref=obuf.at[rows(j * chunk, chunk), :],
                dst_ref=ofull.at[layer, :, pl.ds(pl.multiple_of(cz * BLK, BLK), BLK)],
                send_sem=send_sems.at[m], recv_sem=recv_sems.at[n], device_id=(cx, j, cf), device_id_type=MESH)
            o_tx.append(cp)
        with jax.named_scope('attend'):
            loop(4, attend_all)
        ofull[layer, :, pl.ds(pl.multiple_of(cz * BLK, BLK), BLK)] = obuf[rows(cz * chunk, chunk), :]
        ticks[2]()
        cp_v.wait()
        cp_k.wait()
        with jax.named_scope('wait_o'):
            for cp in o_tx:
                cp.wait_send()
                cp.wait_recv()

    def proj(layer, wo, h_tx):
        loads = []
        for p in QUAD:
            for f in QUAD:
                n = 4 + p * 4 + f
                mine = jnp.logical_and(cz == p, cf == f)

                @pl.when(mine)
                def _():
                    local(wo_ref.at[layer], wo.at[p, f], n)

                @pl.when(jnp.logical_not(mine))
                def _():
                    local(ao_ref.at[layer, p, f], wo.at[p, f], n)
                loads.append(pltpu.make_async_copy(wo_ref.at[layer], wo.at[p, f], loc_sems.at[n]))
        with jax.named_scope('wait_wo'):
            for cp in loads:
                cp.wait()
        gain = gain_row(layer)

        def tile(t):
            r = rows(t * TILE, TILE)
            ot = ofull[layer, r, :]
            parts = []
            for f in QUAD:
                acc = dot_nn(ot[:, 0:BLK], wo[0, f])
                for p in SLOTS:
                    acc = acc + dot_nn(ot[:, p * BLK:(p + 1) * BLK], wo[p, f])
                parts.append(acc.astype(BF16).astype(F32))
            a = jnp.concatenate(parts, axis=1)
            scale = lax.rsqrt(jnp.mean(a * a, axis=-1, keepdims=True) + NORM_EPS)
            hb[r, :] = (hb[r, :].astype(F32) + a * scale * gain).astype(BF16)

        for t in PAIR:
            with jax.named_scope('out_proj'):
                tile(t)
            if layer == 0:
                mark = len(sent)
                h_tx.append((mark, remote([(hb.at[rows(t * TILE, TILE), :], hb.at[rows(chunk + t * TILE, TILE), :])], Y)))

    def mlp_tile(k, t, w, acc, out=None):
        r = rows(t * TILE, TILE)
        ht = hb[r, :]
        gate = dot_nt(ht[:, 0:BLK], w[0, 0])
        up = dot_nt(ht[:, 0:BLK], w[0, 1])
        for f in SLOTS:
            gate = gate + dot_nt(ht[:, f * BLK:(f + 1) * BLK], w[f, 0])
            up = up + dot_nt(ht[:, f * BLK:(f + 1) * BLK], w[f, 1])
        act = (jax.nn.silu(gate) * up).astype(BF16)
        for f in QUAD:
            c = slice(f * BLK, (f + 1) * BLK)
            val = dot_nn(act, w[f, 2])
            if k:
                val = val + acc[r, c]
            if out is None:
                acc[r, c] = val
            else:
                out[rows(t * TILE - chunk, TILE), c] = val.astype(BF16)

    def fetch0(k, wbuf):
        s = k % 2
        p = m0.plane(k)
        cps = []
        for j in QUAD:
            f = (cf + j) % 4
            if k == 0 and j == 0:
                for i, r in enumerate((wg_ref, wu_ref, wd_ref)):
                    cps.append(local(r.at[0, rows(cy * F_HALF, F_HALF), :], wbuf.at[s, f, i], 4 + s * 6 + 3 + i))
            else:
                cps.append(local(aw_ref.at[p, f], wbuf.at[s, f], 4 + s * 6 + (j - 1 if j else 3)))
        return cps

    def fetch1(k, wbuf):
        s = k % 2
        p = m1.plane(k)
        cps = []
        for j in QUAD:
            f = (cf + j) % 4
            if k == 0 and j == 0:
                for i, r in enumerate((wg_ref, wu_ref, wd_ref)):
                    cps.append(local(r.at[1], wbuf.at[s, f, i], 4 + s * 6 + 3 + i))
            else:
                cps.append(local(bw_ref.at[p, f], wbuf.at[s, f], 4 + s * 6 + (j - 1 if j else 3)))
        return cps

    def settle(cps):
        with jax.named_scope('wait_fetch'):
            for cp in cps:
                cp.wait()

    def close(layer, t, m, finish):
        r = rows(t * TILE, TILE)
        m = m.astype(BF16).astype(F32)
        scale = lax.rsqrt(jnp.mean(m * m, axis=-1, keepdims=True) + NORM_EPS)
        hb[r, :] = (hb[r, :].astype(F32) + m * scale * gain_row(2 + layer)).astype(BF16)
        finish(t)

    def mlp0(wbuf, acc, msend, h_tx, ev, finish):
        ev[0]()
        m0.done(0)
        settle(fetch0(0, wbuf))
        with jax.named_scope('mlp0_own'):
            loop(2, lambda t: mlp_tile(0, t, wbuf.at[0], acc))
        ev[7]()
        for _, tx in h_tx:
            arrive(tx, 'wait_h')
        with jax.named_scope('mlp0_other'):
            loop(2, lambda t: mlp_tile(0, t + 2, wbuf.at[0], acc))
        for k in (1, 2):
            ev[k]()
            m0.done(k)
            settle(fetch0(k, wbuf))
            with jax.named_scope('mlp0'):
                loop(4, lambda t: mlp_tile(k, t, wbuf.at[k % 2], acc))
        ev[3]()
        m0.done(3)
        settle(fetch0(3, wbuf))
        m_tx = []
        for t in PAIR:
            with jax.named_scope('mlp0_last'):
                mlp_tile(3, t + 2, wbuf.at[1], acc, msend)
            r = rows(t * TILE, TILE)
            mark = len(sent)
            m_tx.append((mark, remote([(msend.at[r, :], mrecv.at[r, :])], Y)))
        with jax.named_scope('mlp0_own'):
            loop(2, lambda t: mlp_tile(3, t, wbuf.at[1], acc))
        ev[4]()
        for mark, _ in h_tx:
            flush(mark, mark + 1)
        for t in PAIR:
            arrive(m_tx[t][1], f'wait_m_{t}')
            r = rows(t * TILE, TILE)
            close(0, t, acc[r, :] + mrecv[r, :].astype(F32), finish)
            ev[5 + t]()
        for mark, _ in m_tx:
            flush(mark, mark + 1)

    def mlp1(wbuf, acc, ev, finish):
        ev[0]()
        m1.done(0)
        cps = fetch1(0, wbuf)
        for k in QUAD:
            settle(cps)
            if k < 2:
                ev[k + 1]()
                m1.done(k + 1)
                cps = fetch1(k + 1, wbuf)
            if k < 3:
                with jax.named_scope('mlp1'):
                    loop(2, lambda t: mlp_tile(k, t, wbuf.at[k % 2], acc))
                if k == 2:
                    ev[3]()
                    m1.done(3)
                    cps = fetch1(3, wbuf)
            else:
                for t in PAIR:
                    with jax.named_scope('mlp1_last'):
                        mlp_tile(3, t, wbuf.at[1], acc)
                    close(1, t, acc[rows(t * TILE, TILE), :], finish)

    front_scope = dict(wqkv=pltpu.VMEM((3, seq, BLK), BF16), raw=pltpu.VMEM((2, seq, BLK), F32),
                       qkv=pltpu.VMEM((3, seq, BLK), BF16), obuf=pltpu.VMEM((seq, BLK), BF16))
    def nothing():
        pass

    def tick_a():
        m0.got_ya()
        o0.take(S2)
        o0.take(S3)
        m0.take('a', S1)

    def tick_b():
        m0.relay('a', S3)
        o0.got_rx0()

    def mid_a():
        o0.got_xy(S1)
        o0.got_xy(S2)
        m0.take('a', S2)

    def mid_b():
        o0.got_xy(S3)

    def mid_c():
        m0.got_x('a', S1)
        m0.relay('b', S1)
        m0.take('b', S1)

    def tick_c():
        m0.begin_y_rest()
        for k in SLOTS:
            o0.got_r(k)
        o0.done()
        m0.relay('b', S2)

    pl.run_scoped(lambda **kw: front(0, ag_tx=None, ticks=(tick_a, tick_b, tick_c), mid_hooks=(mid_a, mid_b, mid_c), **kw), **front_scope)
    h_tx0 = []
    pl.run_scoped(lambda wo: proj(0, wo, h_tx0), pltpu.VMEM((4, 4, BLK, BLK), BF16))

    def before_own():
        m0.relay('b', S3)
        m0.take('a', S3)
        m0.got_yb()
        m0.got_x('a', S2)
        m0.got_x('b', S1)
        m1.begin_y()
        m1.begin_c()

    def before_other():
        m0.take('b', S2)
        m0.take('b', S3)
        o1.begin()
        for i in TRIO:
            m1.begin_ring(i)
        m0.got_x('a', S3)

    def before_one():
        o1.relay(S1)
        o1.relay(S2)

    def before_two():
        m0.got_x('b', S2)
        o1.relay(S3)

    def before_three():
        m0.got_x('b', S3)
        m1.relay(S1, 0)
        m1.relay(S2, 0)

    def before_sum():
        for i in TRIO:
            m1.got_y0(i)
        m1.take(S1, 0, spread=False)
        for i in TRIO[1:]:
            m1.relay(S2, i)

    def after_first():
        m1.take(S1, TRIO[1], spread=False)

    def after_second():
        q1.begin()
        o1.begin_y()
        m1.take(S1, TRIO[2], spread=False)

    ev0 = (before_own, before_one, before_two, before_three, before_sum, after_first, after_second, before_other)

    ag_marks = []
    ag = [Cast(f'ag_{t}') for t in PAIR]
    fin = [Cast(f'fin_{t}') for t in PAIR]

    def finish0(t):
        blk = rows(cz * chunk + t * TILE, TILE)
        mark = len(sent)
        ag[t].push(0, [(hb.at[rows(t * TILE, TILE), :], xbuf.at[blk, :])])
        ag_marks.append((mark, len(sent)))
        xbuf[blk, :] = hb[rows(t * TILE, TILE), :]

    pl.run_scoped(lambda wbuf, acc, msend: mlp0(wbuf, acc, msend, h_tx0, ev0, finish0),
                  pltpu.VMEM((2, 4, 3, F_HALF, BLK), BF16), pltpu.VMEM((2 * chunk, 2048), F32), pltpu.VMEM((chunk, 2048), BF16))

    def ag_block(k, t):
        return xbuf.at[rows(slot_plane(k) * chunk + t * TILE, TILE), :]

    def ag_relay(k):
        for t in PAIR:
            ag[t].relay(k, same([ag_block(k, t)]))

    def ag_part(k):
        if k == S2:
            ag_relay(S3)
            for i in TRIO[1:]:
                m1.relay(S1, i)
            m1.got_r0()
            o1.got_xy(S1)
            o1.got_rx0()
            for i in TRIO:
                m1.got_xy(S1, i)
                m1.take(S2, i)
        for t in PAIR:
            ag[t].take(k)
        if k == S3:
            o1.got_xy(S2)
            o1.got_xy(S3)

    def front_one(**kw):
        for t in PAIR:
            for k in (S1, S2):
                ag[t].relay(k, same([ag_block(k, t)]))
        for i in TRIO:
            q1.got_y(i)
        for k in SLOTS:
            o1.take(k)
        o1.got_y0()
        for i in TRIO:
            m1.spread(S1, i)
        for i in TRIO:
            q1.got_r(i)
        q1.done()
        front(1, ag_tx=lambda k: ag_part(k) if k else None, ticks=(tick_d, tick_e, tick_f), mid_hooks=(mid_d, mid_e, mid_f), **kw)

    def tick_d():
        for i in TRIO:
            m1.relay(S3, i)

    def tick_e():
        for i in TRIO:
            m1.got_r(S1, i)

    def mid_d():
        for i in TRIO:
            m1.got_xy(S2, i)

    def mid_e():
        m1.take(S3, 0)

    def mid_f():
        m1.take(S3, TRIO[1])

    def tick_f():
        for k in SLOTS:
            o1.got_r(k)
        o1.done()
        for i in TRIO:
            m1.got_r(S2, i)
        m1.take(S3, TRIO[2])
        m1.got_xy(S3, 0)
        m1.got_xy(S3, TRIO[1])

    pl.run_scoped(front_one, **front_scope)
    for first, last in ag_marks:
        flush(first, last)
    pl.run_scoped(lambda wo: proj(1, wo, None), pltpu.VMEM((4, 4, BLK, BLK), BF16))

    def last_relays():
        m1.got_xy(S3, TRIO[2])
        m1.got_r(S3, 0)

    def last_blocks():
        for i in TRIO[1:]:
            m1.got_r(S3, i)

    ev1 = (last_relays, nothing, nothing, last_blocks)

    def finish1(t):
        blk = rows(cz * chunk + t * TILE, TILE)
        fin[t].push(0, [(hb.at[rows(t * TILE, TILE), :], y_ref.at[blk, :])])
        local(hb.at[rows(t * TILE, TILE), :], y_ref.at[blk, :], 1 + t)

    pl.run_scoped(lambda wbuf, acc: mlp1(wbuf, acc, ev1, finish1),
                  pltpu.VMEM((2, 4, 3, 1376, BLK), BF16), pltpu.VMEM((chunk, 2048), F32))
    def fin_block(k, t):
        return y_ref.at[rows(slot_plane(k) * chunk + t * TILE, TILE), :]

    for k in SLOTS:
        for t in PAIR:
            fin[t].relay(k, same([fin_block(k, t)]))
    for k in SLOTS:
        for t in PAIR:
            fin[t].take(k)
    for t in PAIR:
        pltpu.make_async_copy(hb.at[rows(t * TILE, TILE), :], y_ref.at[rows(t * TILE, TILE), :], loc_sems.at[1 + t]).wait()
    flush()
    assert max(state.values()) <= N_SEM, state


def mega_call(x, wq, wk, wv, wo, wg, wu, wd, gains, tab):
    seq, width = x.shape
    any_spec = pl.BlockSpec(memory_space=pl.ANY)
    chunk = seq // 4
    outs = [jax.ShapeDtypeStruct((seq, width), BF16),
            jax.ShapeDtypeStruct((2, seq, BLK), BF16), jax.ShapeDtypeStruct((2, seq, BLK), BF16),
            jax.ShapeDtypeStruct((2, 3, 2048, BLK), BF16), jax.ShapeDtypeStruct((2, 4, 4, BLK, BLK), BF16),
            jax.ShapeDtypeStruct((4, 4, 3, F_HALF, BLK), BF16), jax.ShapeDtypeStruct((4, 4, 3, 1376, BLK), BF16)]
    return pl.pallas_call(
        mega,
        in_specs=[any_spec] * 10,
        out_specs=[any_spec] * 7,
        out_shape=outs,
        scratch_shapes=[pltpu.VMEM((seq, width), BF16), pltpu.VMEM((2 * chunk, width), BF16)] + [pltpu.VMEM((chunk, width), BF16)] + [
                        pltpu.VMEM((2, chunk, width), BF16), pltpu.VMEM((2, 4, 8, seq), F32),
                        pltpu.VMEM((seq, LANE), F32), pltpu.VMEM((seq, LANE), F32), pltpu.VMEM((4, 8, BLK), F32),
                        pltpu.SemaphoreType.DMA((N_SEM,)), pltpu.SemaphoreType.DMA((N_SEM,)),
                        pltpu.SemaphoreType.DMA((32,))],
        compiler_params=pltpu.CompilerParams(has_side_effects=True, vmem_limit_bytes=67043328),
        name='mega')(x, wq, wk, wv, wo, wg, wu, wd, gains, tab)


def solution(mesh):
    batch_axes = ('dp', 'fsdp')
    act_spec = P(batch_axes, None, None)
    in_cols = P(None, 'fsdp', 'tp')
    in_rows = P(None, 'tp', 'fsdp')
    tp_gain = P(None, 'tp')
    fsdp_gain = P(None, 'fsdp')
    cache_spec = P(None, batch_axes, None, 'tp', None)

    def local_layers(x, w_query, w_key, w_value, w_out, w_gate, w_up, w_down, q_norm_w, k_norm_w, attn_norm_w, ffn_norm_w):
        batch, seq_len, width = x.shape
        gains = jnp.concatenate([attn_norm_w, ffn_norm_w, q_norm_w, k_norm_w], axis=0)
        tab = jnp.asarray(rope_table(seq_len))
        outs = mega_call(x.reshape(seq_len, width), w_query, w_key, w_value, w_out,
                         jnp.swapaxes(w_gate, 1, 2), jnp.swapaxes(w_up, 1, 2), w_down, gains, tab)
        shape = (2, 1, seq_len, 4, HEAD_DIM)
        return outs[0].reshape(x.shape), outs[1].reshape(shape), outs[2].reshape(shape)

    return jax.shard_map(local_layers, mesh=mesh,
                         in_specs=(act_spec, in_cols, in_cols, in_cols, in_rows, in_cols, in_cols, in_rows,
                                   tp_gain, tp_gain, fsdp_gain, fsdp_gain),
                         out_specs=(act_spec, cache_spec, cache_spec), check_vma=False)
```

```python
import functools
import jax
import jax.numpy as jnp
import numpy as np
from jax import lax
from jax.experimental import pallas as pl
from jax.experimental.pallas import tpu as pltpu
from jax.sharding import PartitionSpec as P

HEAD_DIM = 128
NORM_EPS = 1e-6
ROPE_THETA = 500000.0
LOG2E = 1.4426950408889634
MESH = pl.DeviceIdType.MESH
BF16 = jnp.bfloat16
F32 = jnp.float32
N_SEM = 300
TILE = 256
BLK = 512
LANE = 128
F_HALF = 688
S1, S2, S3 = SLOTS = (1, 2, 3)
PAIR = range(2)
TRIO = range(3)
QUAD = range(4)
ALL = slice(None)


def rope_table(seq_len):
    half = HEAD_DIM // 2
    inv_freq = np.float32(ROPE_THETA) ** (-2.0 * np.arange(half, dtype=np.float32) / np.float32(HEAD_DIM))
    angles = np.arange(seq_len, dtype=np.float32)[:, None] * inv_freq.astype(np.float32)[None, :]
    return np.concatenate([np.cos(angles), np.sin(angles)], axis=1).astype(np.float32)


def dot_nt(lhs, rhs):
    return lax.dot_general(lhs, rhs, (((1,), (1,)), ((), ())), preferred_element_type=F32)


def dot_nn(lhs, rhs):
    return jnp.dot(lhs, rhs, preferred_element_type=F32)


def loop(count, body):
    lax.fori_loop(0, count, lambda i, c: (body(i), c)[1], 0)


def mega(x_ref, wq_ref, wk_ref, wv_ref, wo_ref, wg_ref, wu_ref, wd_ref, gain_ref, tab_ref,
         y_ref, kc_ref, vc_ref, aq_ref, ao_ref, aw_ref, bw_ref,
         xbuf, hb, mrecv, ofull, sqb, cosb, sinb, gp, send_sems, recv_sems, loc_sems):
    seq = x_ref.shape[0]
    chunk = seq // 4
    cx, cz, cf = lax.axis_index('dp'), lax.axis_index('tp'), lax.axis_index('fsdp')
    cy = cf // 2
    f1 = cf + 1 - 2 * (cf % 2)
    f2 = (cf + 2) % 4
    nx = 1 - cx
    X = (nx, cz, cf)
    Y = (cx, cz, f2)
    C = (cx, cz, f1)
    mid = (cz + 1) // 2 == 1
    half_z = cz // 2
    outer = 3 * half_z
    state = {'send': 0, 'recv': 0}
    sent = []

    def take_number(kind):
        state[kind] += 1
        return state[kind] - 1

    def frozen(ref):
        if not getattr(ref, 'transforms', ()):
            return ref, None
        idx, = ref.transforms
        return ref.ref, tuple(int(i.size) if isinstance(i, pl.Slice) else None for i in idx.indices)

    def thawed(item):
        ref, sizes = item
        return ref if sizes is None else ref.at[tuple(0 if s is None else pl.ds(0, s) for s in sizes)]

    def expect(pairs):
        return [(take_number('recv'), frozen(dst)) for _, dst in pairs]

    def remote(pairs, dev, into=None, when=None):
        pairs = list(pairs)
        into = expect(pairs) if into is None else into
        for (src, dst), (n, _) in zip(pairs, into):
            m = take_number('send')
            cp = pltpu.make_async_remote_copy(src_ref=src, dst_ref=dst, send_sem=send_sems.at[m], recv_sem=recv_sems.at[n],
                                              device_id=dev, device_id_type=MESH)
            cp.start()
            sent.append((m, frozen(src), when))
        return into

    def handle(ref, m, n):
        return pltpu.make_async_remote_copy(src_ref=thawed(ref), dst_ref=thawed(ref), send_sem=send_sems.at[m],
                                            recv_sem=recv_sems.at[n], device_id=(0, 0, 0), device_id_type=MESH)

    def arrive(cps, name='recv'):
        with jax.named_scope(name):
            for n, ref in cps:
                handle(ref, 0, n).wait_recv()

    def flush(first=0, last=None):
        for m, ref, when in sent[first:last]:
            if m in flushed:
                continue
            flushed.add(m)
            if when is None:
                handle(ref, m, 0).wait_send()
            else:
                @pl.when(mid if when == 'mid' else jnp.logical_not(mid))
                def _():
                    handle(ref, m, 0).wait_send()

    flushed = set()

    def slot_plane(k):
        return (cz, 1 - cz + 4 * half_z, 2 - half_z, 3 - 3 * half_z)[k]

    class Cast:
        def __init__(self, name):
            self.name, self.slots, self.heard = name, None, set()

        def push(self, k, pairs):
            pairs = list(pairs)
            if self.slots is None:
                self.slots = [None] + [expect(pairs) for _ in TRIO]

            @pl.when(mid)
            def _():
                if k < 2:
                    remote(pairs, (cx, 3 - cz, cf), self.slots[2 + k], 'mid')
                if k != 1:
                    remote(pairs, (cx, outer, cf), self.slots[max(k, 1)], 'mid')
            if k == 0:
                @pl.when(jnp.logical_not(mid))
                def _():
                    remote(pairs, (cx, 1 + half_z, cf), self.slots[1], 'end')

        def hear(self, k):
            if k not in self.heard:
                self.heard.add(k)

                @pl.when(mid)
                def _():
                    arrive(self.slots[k], f'relay_{self.name}_{k}')

        def relay(self, k, pairs):
            self.hear(k)
            self.push(k, pairs)

        def take(self, k):
            self.hear(k)

            @pl.when(jnp.logical_not(mid))
            def _():
                arrive(self.slots[k], f'take_{self.name}_{k}')

    def rows(base, size):
        return pl.ds(base if isinstance(base, int) else pl.multiple_of(base, 16), size)

    def cols(base, size):
        return pl.ds(base if isinstance(base, int) else pl.multiple_of(base, LANE), size)

    def same(refs):
        return list(zip(refs, refs))

    class Group:
        def __init__(self, kind, layer):
            self.kind, self.layer, self.tx = kind, layer, {}

        def plane(self, k):
            return slot_plane(k)

        def cast(self, key):
            name = f'{self.kind}{self.layer}{key}'
            return self.tx.setdefault('cast' + key, Cast(name))

        def wait(self, *keys):
            for key in keys:
                arrive(self.tx[key], f'wait_{self.kind}{self.layer}_{key}')

        def send(self, key, pairs, dev):
            self.tx[key] = remote(pairs, dev)

    class QGroup(Group):
        def whole(self, i, f):
            return aq_ref.at[self.layer, i, rows(f * BLK, BLK), :]

        def half(self, i, f):
            return aq_ref.at[self.layer, i, rows(f * BLK + cx * TILE, TILE), :]

        def begin(self):
            own = (wq_ref, wk_ref, wv_ref)
            for i in TRIO:
                self.send(f'y{i}', [(own[i].at[self.layer, rows(cx * TILE, TILE), :], self.half(i, cf))], Y)
            for i in TRIO:
                self.send(f'c{i}', [(own[i].at[self.layer], self.whole(i, cf))], C)

        def got_y(self, i):
            self.wait(f'y{i}')
            self.send(f'r{i}', same([self.half(i, f2)]), X)

        def got_r(self, i):
            self.wait(f'r{i}')
            self.send(f'd{i}', same([self.whole(i, f2)]), C)

        def done(self):
            for i in TRIO:
                self.wait(f'c{i}', f'd{i}')

    class OGroup(Group):
        def whole(self, p, f):
            return ao_ref.at[self.layer, p, f]

        def part(self, p, f, first, size):
            return ao_ref.at[self.layer, p, f, rows(first, size), :]

        def begin(self):
            half = self.part(cz, cf, cx * TILE, TILE)
            src = wo_ref.at[self.layer, rows(cx * TILE, TILE), :]
            self.cast('').push(0, [(src, half)])

        def begin_y(self):
            own, half = wo_ref.at[self.layer], self.part(cz, cf, cx * TILE, TILE)
            src = wo_ref.at[self.layer, rows(cx * TILE, TILE), :]
            self.send('y0', [(src, half)], Y)
            self.send('c0', [(own, self.whole(cz, cf))], C)

        def got_y0(self):
            self.wait('y0')
            self.send('rx0', same([self.part(cz, f2, cx * TILE, TILE)]), X)

        def got_rx0(self):
            self.wait('rx0')
            self.send('d0', same([self.whole(cz, f2)]), C)

        def relay(self, k):
            self.cast('').relay(k, same([self.part(self.plane(k), cf, cx * TILE, TILE)]))

        def take(self, k):
            self.cast('').take(k)
            refs = same([self.part(self.plane(k), cf, cx * TILE, TILE)])
            self.send(f'x{k}', refs, X)
            self.send(f'y{k}', refs, Y)

        def got_xy(self, k):
            p = self.plane(k)
            self.wait(f'x{k}')
            self.send(f'ry{k}', same([self.part(p, cf, nx * TILE + LANE, LANE)]), Y)
            self.send(f'c{k}', same([self.whole(p, cf)]), C)
            self.wait(f'y{k}')
            self.send(f'rx{k}', same([self.part(p, f2, cx * TILE, LANE)]), X)

        def got_r(self, k):
            self.wait(f'rx{k}', f'ry{k}')
            self.send(f'd{k}', same([self.whole(self.plane(k), f2)]), C)

        def done(self):
            for k in QUAD:
                self.wait(f'c{k}', f'd{k}')

    class MGroup(Group):
        def whole(self, p, f):
            return aw_ref.at[p, f]

        def lane(self, p, f, i):
            return aw_ref.at[p, f, i, :, cols(cx * TILE, TILE)]

        def first(self, f, xh, own_y, i):
            src = (wg_ref, wu_ref, wd_ref)[i].at[self.layer, rows(own_y * F_HALF, F_HALF), cols(xh * TILE, TILE)]
            return src, aw_ref.at[cz, f, i, :, cols(xh * TILE, TILE)]

        def begin_ring(self):
            self.cast('a').push(0, [self.first(cf, cx, cy, i) for i in TRIO])

        def begin_y(self):
            self.send('ya', [self.first(cf, cx, 1 - cy, i) for i in TRIO], Y)

        def begin_y_rest(self):
            self.send('yb', [self.first(cf, nx, 1 - cy, i) for i in TRIO], Y)

        def begin_c(self):
            self.send('c0', [((wg_ref, wu_ref, wd_ref)[i].at[self.layer, rows(cy * F_HALF, F_HALF), :], aw_ref.at[cz, cf, i])
                             for i in TRIO], C)

        def got_ya(self):
            self.wait('ya')
            self.cast('b').push(0, same([self.lane(cz, f2, i) for i in TRIO]))

        def got_yb(self):
            self.wait('yb')
            self.send('d0', same([self.whole(cz, f2)]), C)

        def relay(self, ab, k):
            f = cf if ab == 'a' else f2
            self.cast(ab).relay(k, same([self.lane(self.plane(k), f, i) for i in TRIO]))

        def take(self, ab, k):
            self.cast(ab).take(k)
            f = cf if ab == 'a' else f2
            self.send(f'x{ab}{k}', same([self.lane(self.plane(k), f, i) for i in TRIO]), X)

        def got_x(self, ab, k):
            self.wait(f'x{ab}{k}')
            self.send(f"{'c' if ab == 'a' else 'd'}{k}", same([self.whole(self.plane(k), cf if ab == 'a' else f2)]), C)

        def done(self, k):
            self.wait(f'c{k}', f'd{k}')

    class WideGroup(Group):
        def srcs(self):
            return [r.at[self.layer, rows(cx * F_HALF, F_HALF), :] for r in (wg_ref, wu_ref, wd_ref)]

        def block(self, p, f, i):
            return bw_ref.at[p, f, i]

        def half(self, p, f, xh, i):
            return bw_ref.at[p, f, i, rows(xh * F_HALF, F_HALF), :]

        def quarter(self, p, f, xh, i, side):
            return bw_ref.at[p, f, i, rows(xh * F_HALF, F_HALF), pl.ds(side * TILE, TILE)]

        def begin_ring(self, i):
            self.cast(f'{i}').push(0, [(self.srcs()[i], self.half(cz, cf, cx, i))])

        def begin_y(self):
            for i in TRIO:
                self.send(f'y0{i}', [(self.srcs()[i], self.half(cz, cf, cx, i))], Y)

        def begin_c(self):
            own = [r.at[self.layer] for r in (wg_ref, wu_ref, wd_ref)]
            self.send('c0', [(own[i], self.block(cz, cf, i)) for i in TRIO], C)

        def got_y0(self, i):
            self.wait(f'y0{i}')
            self.send(f'r0{i}', same([self.half(cz, f2, cx, i)]), X)

        def got_r0(self):
            self.wait('r00', 'r01', 'r02')
            self.send('d0', same([bw_ref.at[cz, f2]]), C)

        def relay(self, k, i):
            self.cast(f'{i}').relay(k, same([self.half(self.plane(k), cf, cx, i)]))

        def take(self, k, i, spread=True):
            self.cast(f'{i}').take(k)
            self.send(f'x{k}{i}', same([self.half(self.plane(k), cf, cx, i)]), X)
            if spread:
                self.spread(k, i)

        def spread(self, k, i):
            self.send(f'y{k}{i}', same([self.half(self.plane(k), cf, cx, i)]), Y)

        def got_xy(self, k, i):
            p = self.plane(k)
            self.wait(f'x{k}{i}')
            self.send(f'ry{k}{i}', same([self.quarter(p, cf, nx, i, 1)]), Y)
            self.send(f'c{k}{i}', same([self.block(p, cf, i)]), C)
            self.wait(f'y{k}{i}')
            self.send(f'rx{k}{i}', same([self.quarter(p, f2, cx, i, 0)]), X)

        def got_r(self, k, i):
            self.wait(f'rx{k}{i}', f'ry{k}{i}')
            self.send(f'd{k}{i}', same([self.block(self.plane(k), f2, i)]), C)

        def done(self, k):
            if k == 0:
                self.wait('c0', 'd0')
            else:
                for i in TRIO:
                    self.done_part(k, i)

        def done_part(self, k, i):
            self.wait(f'c{k}{i}', f'd{k}{i}')

    def local(src, dst, n):
        cp = pltpu.make_async_copy(src, dst, loc_sems.at[n])
        cp.start()
        return cp

    gate_sem = pltpu.get_barrier_semaphore()
    partners = [X] + [(cx, cz, (cf + off) % 4) for off in SLOTS] + [(cx, (cz + off) % 4, cf) for off in SLOTS]
    for dev in partners:
        pl.semaphore_signal(gate_sem, inc=1, device_id=dev, device_id_type=MESH)
    pl.semaphore_wait(gate_sem, len(partners))

    q0, o0, m0 = QGroup('q', 0), OGroup('o', 0), MGroup('m', 0)
    q1, o1, m1 = QGroup('q', 1), OGroup('o', 1), WideGroup('m', 1)

    o0.begin()
    gain_tx = []
    for off in SLOTS:
        gain_tx.append(remote([(gain_ref, gp.at[cf])], (cx, cz, (cf + off) % 4)))
    q0.begin()
    o0.begin_y()
    m0.begin_y()
    m0.begin_c()
    ld_x = local(x_ref, xbuf, 0)
    ld_g = local(gain_ref, gp.at[cf], 1)
    ld_t = local(tab_ref, cosb, 2)
    ld_h = local(x_ref.at[rows(cz * chunk, chunk), :], hb.at[rows(0, chunk), :], 3)
    ld_t.wait()

    def make_tables(i):
        r = rows(i * TILE, TILE)
        tab = cosb[r, :]
        rolled = pltpu.roll(tab, 64, 1)
        low = lax.broadcasted_iota(jnp.int32, (TILE, LANE), 1) < 64
        cosb[r, :] = jnp.where(low, tab, rolled)
        sinb[r, :] = jnp.where(low, -rolled, tab)

    with jax.named_scope('tables'):
        loop(seq // TILE, make_tables)

    o0.relay(S1)
    o0.relay(S2)
    m0.begin_ring()
    o0.take(S1)
    for i in TRIO:
        q0.got_y(i)
    o0.relay(S3)
    o0.got_y0()
    for i in TRIO:
        q0.got_r(i)
    for tx in gain_tx:
        arrive(tx)
    q0.done()
    m0.relay('a', S1)
    m0.relay('a', S2)
    ld_x.wait()
    ld_g.wait()
    ld_h.wait()

    def gain_row(i):
        return jnp.concatenate([gp[f, i:i + 1, :] for f in QUAD], axis=1)

    o_recv = [[], []]

    def front(layer, wqkv, raw, qkv, obuf, ag_tx, ticks, mid_hooks):
        loads = [local(aq_ref.at[layer, i, rows(((cf + j) % 4) * BLK, BLK), :],
                       wqkv.at[i, rows(((cf + j) % 4) * BLK, BLK), :], 4 + i * 4 + j) for i in TRIO for j in SLOTS]
        loads += [local(r.at[layer], wqkv.at[i, rows(cf * BLK, BLK), :], 4 + i * 4)
                  for i, r in enumerate((wq_ref, wk_ref, wv_ref))]
        with jax.named_scope('wait_wqkv'):
            for cp in loads:
                cp.wait()
        lane = lax.broadcasted_iota(jnp.int32, (TILE, LANE), 1)

        def project(t):
            r = rows(t * TILE, TILE)
            xt = xbuf[r, :]
            qv = dot_nn(xt, wqkv[0])
            raw[0, r, :] = qv
            kv = dot_nn(xt, wqkv[1])
            raw[1, r, :] = kv
            qkv[2, r, :] = dot_nn(xt, wqkv[2]).astype(BF16)
            qs = jnp.sum(qv * qv, axis=-1, keepdims=True)
            ks = jnp.sum(kv * kv, axis=-1, keepdims=True)
            both = jnp.where(lane == 0, qs, jnp.where(lane == 1, ks, 0.0))
            sqb[layer, cz, :, pl.ds(pl.multiple_of(t * TILE, TILE), TILE)] = both.T[0:8, :]

        if ag_tx is None:
            with jax.named_scope('project'):
                loop(seq // TILE, project)
        else:
            for s in QUAD:
                ag_tx(s)
                base = slot_plane(s) * 2
                with jax.named_scope('project'):
                    loop(2, lambda t: project(base + t))
        sq_tx = []
        for off in SLOTS:
            ref = sqb.at[layer, cz]
            sq_tx.append(remote([(ref, ref)], (cx, (cz + off) % 4, cf)))
        cp_v = local(qkv.at[2], vc_ref.at[layer], 20)
        ticks[0]()
        for tx in sq_tx:
            arrive(tx, 'wait_sq')

        def rope(t):
            r = rows(t * TILE, TILE)
            c = pl.ds(pl.multiple_of(t * TILE, TILE), TILE)
            tot = sqb[layer, 0, :, c] + sqb[layer, 1, :, c] + sqb[layer, 2, :, c] + sqb[layer, 3, :, c]
            inv = lax.rsqrt(tot * (1.0 / (4 * BLK)) + NORM_EPS)
            cols = jnp.concatenate([inv] * 16, axis=0).T
            cos_t, sin_t = cosb[r, :], sinb[r, :]
            for i in PAIR:
                scale = cols[:, i:i + 1]
                for h in QUAD:
                    hs = slice(h * LANE, (h + 1) * LANE)
                    val = raw[i, r, hs] * scale * gp[cf, 4 + 2 * i + layer:5 + 2 * i + layer, hs]
                    qkv[i, r, hs] = (val * cos_t + pltpu.roll(val, 64, 1) * sin_t).astype(BF16)

        with jax.named_scope('rope'):
            loop(seq // TILE, rope)
        cp_k = local(qkv.at[1], kc_ref.at[layer], 21)
        ticks[1]()
        order = (2, 1, 3, 0)
        bq = TILE
        sm = (HEAD_DIM ** -0.5) * LOG2E
        o_tx = []

        def attend(off):
            j = (cz + off) % 4

            def step(it):
                h, sub = it // 2, it % 2
                i = 2 * j + sub
                hc = pl.ds(pl.multiple_of(h * LANE, LANE), LANE)
                for n in range(seq // bq):
                    @pl.when(i == n)
                    def _():
                        q_blk = qkv[0, n * bq:(n + 1) * bq, hc]
                        diag = dot_nt(q_blk, qkv[1, n * bq:(n + 1) * bq, hc])
                        ri = lax.broadcasted_iota(jnp.int32, (bq, bq), 0)
                        ci = lax.broadcasted_iota(jnp.int32, (bq, bq), 1)
                        diag = jnp.where(ri >= ci, diag, -jnp.inf)
                        top = jnp.max(diag, axis=-1, keepdims=True)
                        if n:
                            full = dot_nt(q_blk, qkv[1, 0:n * bq, hc])
                            top = jnp.maximum(top, jnp.max(full, axis=-1, keepdims=True))
                        e_diag = jnp.exp2((diag - top) * sm)
                        total = jnp.sum(e_diag, axis=-1, keepdims=True)
                        if n:
                            e_full = jnp.exp2((full - top) * sm)
                            total = total + jnp.sum(e_full, axis=-1, keepdims=True)
                        inv = 1.0 / total
                        out = dot_nn((e_diag * inv).astype(BF16), qkv[2, n * bq:(n + 1) * bq, hc])
                        if n:
                            out = out + dot_nn((e_full * inv).astype(BF16), qkv[2, 0:n * bq, hc])
                        obuf[n * bq:(n + 1) * bq, hc] = out.astype(BF16)

            loop(8, step)

        def attend_all(g):
            off = jnp.where(g == 0, 2, jnp.where(g == 1, 1, jnp.where(g == 2, 3, 0)))
            attend(off)
            for gi, o in enumerate(order[:3]):
                @pl.when(g == gi)
                def _():
                    o_tx[gi].start()
                    mid_hooks[gi]()

        for o in order[:3]:
            m, n = take_number('send'), take_number('recv')
            j = (cz + o) % 4
            cp = pltpu.make_async_remote_copy(
                src_ref=obuf.at[rows(j * chunk, chunk), :],
                dst_ref=ofull.at[:, pl.ds(pl.multiple_of(cz * BLK, BLK), BLK)],
                send_sem=send_sems.at[m], recv_sem=recv_sems.at[n], device_id=(cx, j, cf), device_id_type=MESH)
            o_tx.append(cp)
            o_recv[layer].append((n, frozen(ofull.at[:, pl.ds(0, BLK)])))
        with jax.named_scope('attend'):
            loop(4, attend_all)
        ofull[:, pl.ds(pl.multiple_of(cz * BLK, BLK), BLK)] = obuf[rows(cz * chunk, chunk), :]
        ticks[2]()
        cp_v.wait()
        cp_k.wait()
        for cp in o_tx:
            cp.wait_send()

    def wo_waits(layer, wo_at):
        return [pltpu.make_async_copy(wo_ref.at[layer], wo_at(n), loc_sems.at[40 + n]) for n in range(16)]

    def wo_loads(layer, wo_at):
        for n in range(16):
            p, f = n // 4, n % 4
            mine = jnp.logical_and(cz == p, cf == f)

            @pl.when(mine)
            def _():
                local(wo_ref.at[layer], wo_at(n), 40 + n)

            @pl.when(jnp.logical_not(mine))
            def _():
                local(ao_ref.at[layer, p, f], wo_at(n), 40 + n)

    def wo_in_x(n):
        return xbuf.at[rows(n // 4 * BLK, BLK), pl.ds(n % 4 * BLK, BLK)]

    def proj(layer, wo_at, loads, h_tx):
        arrive(o_recv[layer], 'wait_o')
        with jax.named_scope('wait_wo'):
            for cp in loads:
                cp.wait()
        gain = gain_row(layer)

        def tile(t):
            r = rows(t * TILE, TILE)
            ot = ofull[r, :]
            parts = []
            for f in QUAD:
                acc = dot_nn(ot[:, 0:BLK], wo_at(f)[...])
                for p in SLOTS:
                    acc = acc + dot_nn(ot[:, p * BLK:(p + 1) * BLK], wo_at(p * 4 + f)[...])
                parts.append(acc.astype(BF16).astype(F32))
            a = jnp.concatenate(parts, axis=1)
            scale = lax.rsqrt(jnp.mean(a * a, axis=-1, keepdims=True) + NORM_EPS)
            hb[r, :] = (hb[r, :].astype(F32) + a * scale * gain).astype(BF16)

        for t in PAIR:
            with jax.named_scope('out_proj'):
                tile(t)
            if layer == 0:
                mark = len(sent)
                h_tx.append((mark, remote([(hb.at[rows(t * TILE, TILE), :], hb.at[rows(chunk + t * TILE, TILE), :])], Y)))

    def mlp_act(t, w):
        ht = hb[rows(t * TILE, TILE), :]
        gate = dot_nt(ht[:, 0:BLK], w[0, 0])
        up = dot_nt(ht[:, 0:BLK], w[0, 1])
        for f in range(1, 4):
            gate = gate + dot_nt(ht[:, f * BLK:(f + 1) * BLK], w[f, 0])
            up = up + dot_nt(ht[:, f * BLK:(f + 1) * BLK], w[f, 1])
        return (jax.nn.silu(gate) * up).astype(BF16)

    def mlp_down(first, t, act, w, acc, out=None):
        r = rows(t * TILE, TILE)
        for f in QUAD:
            c = slice(f * BLK, (f + 1) * BLK)
            val = dot_nn(act, w[f, 2])
            if not first:
                val = val + acc[r, c]
            if out is None:
                acc[r, c] = val
            else:
                out[rows(t * TILE - chunk, TILE), c] = val.astype(BF16)

    def mlp_tile(first, t, w, acc, out=None):
        mlp_down(first, t, mlp_act(t, w), w, acc, out)

    def fetch0(k, wbuf):
        s = k % 2
        p = m0.plane(k)
        cps = []
        for j in QUAD:
            f = (cf + j) % 4
            if k == 0 and j == 0:
                for i, r in enumerate((wg_ref, wu_ref, wd_ref)):
                    cps.append(local(r.at[0, rows(cy * F_HALF, F_HALF), :], wbuf.at[s, f, i], 4 + s * 6 + 3 + i))
            else:
                cps.append(local(aw_ref.at[p, f], wbuf.at[s, f], 4 + s * 6 + (j - 1 if j else 3)))
        return cps

    def fetch1(k, s, wbuf):
        p = m1.plane(k)
        cps = []
        for j in QUAD:
            f = (cf + j) % 4
            if k == 0 and j == 0:
                for i, r in enumerate((wg_ref, wu_ref, wd_ref)):
                    cps.append(local(r.at[1], wbuf.at[s, f, i], 4 + s * 6 + 3 + i))
            else:
                cps.append(local(bw_ref.at[p, f], wbuf.at[s, f], 4 + s * 6 + (j - 1 if j else 3)))
        return cps

    def settle(cps):
        with jax.named_scope('wait_fetch'):
            for cp in cps:
                cp.wait()

    def close(layer, t, m, finish):
        r = rows(t * TILE, TILE)
        m = m.astype(BF16).astype(F32)
        scale = lax.rsqrt(jnp.mean(m * m, axis=-1, keepdims=True) + NORM_EPS)
        hb[r, :] = (hb[r, :].astype(F32) + m * scale * gain_row(2 + layer)).astype(BF16)
        finish(t)

    def mlp0(wbuf, acc, msend, h_tx, ev, finish):
        ev[0]()
        m0.done(0)
        settle(fetch0(0, wbuf))
        with jax.named_scope('mlp0_own'):
            loop(2, lambda t: mlp_tile(True, t, wbuf.at[0], acc))
        ev[7]()
        for _, tx in h_tx:
            arrive(tx, 'wait_h')
        with jax.named_scope('mlp0_other'):
            loop(2, lambda t: mlp_tile(True, t + 2, wbuf.at[0], acc))
        for k in (1, 2):
            ev[k]()
            m0.done(k)
            settle(fetch0(k, wbuf))
            with jax.named_scope('mlp0'):
                loop(4, lambda t: mlp_tile(False, t, wbuf.at[k % 2], acc))
        ev[3]()
        m0.done(3)
        settle(fetch0(3, wbuf))
        m_tx = []
        for t in PAIR:
            with jax.named_scope('mlp0_last'):
                mlp_tile(False, t + 2, wbuf.at[1], acc, msend)
            r = rows(t * TILE, TILE)
            mark = len(sent)
            m_tx.append((mark, remote([(msend.at[r, :], mrecv.at[r, :])], Y)))
        with jax.named_scope('mlp0_own'):
            loop(2, lambda t: mlp_tile(False, t, wbuf.at[1], acc))
        ev[4]()
        for mark, _ in h_tx:
            flush(mark, mark + 1)
        for t in PAIR:
            arrive(m_tx[t][1], f'wait_m_{t}')
            r = rows(t * TILE, TILE)
            close(0, t, acc[r, :] + mrecv[r, :].astype(F32), finish)
            ev[5 + t]()
        for mark, _ in m_tx:
            flush(mark, mark + 1)

    def mlp1(wbuf, acc, finish):
        spare = (rows(chunk, TILE), pl.ds(0, 2 * F_HALF))

        def run(k, slot, t, first=False):
            with jax.named_scope(f'mlp1_{t}_{k}'):
                mlp_tile(first, t, wbuf.at[slot], acc)

        m1.done(0)
        cps = fetch1(0, 0, wbuf)
        proj(1, wo_in_x, wo_waits(1, wo_in_x), None)
        m1.take(S3, S2)
        m1.done(S1)
        settle(cps)
        cps = fetch1(S1, 1, wbuf)
        run(0, 0, 0, True)
        settle(cps)
        m1.done(S2)
        cps = fetch1(S2, 0, wbuf)
        run(S1, 1, 0)
        for i in PAIR:
            m1.got_r(S3, i)
        settle(cps)
        run(S2, 0, 0)
        m1.got_xy(S3, S2)
        p = m1.plane(S3)
        for i in PAIR:
            m1.done_part(S3, i)
        settle([local(bw_ref.at[p, f, pl.ds(0, 2)], wbuf.at[1, f, pl.ds(0, 2)], 4 + f) for f in QUAD])
        with jax.named_scope('mlp1_act'):
            hb[spare] = mlp_act(0, wbuf.at[1])
        m1.got_r(S3, S2)
        m1.done_part(S3, S2)
        settle([local(bw_ref.at[p, f, S2], wbuf.at[1, f, S2], 4 + f) for f in QUAD])
        with jax.named_scope('mlp1_down'):
            mlp_down(False, 0, hb[spare], wbuf.at[1], acc)
        close(1, 0, acc[rows(0, TILE), :], finish)
        run(S2, 0, 1, True)
        cps = fetch1(0, 0, wbuf)
        run(S3, 1, 1)
        settle(cps)
        cps = fetch1(S1, 1, wbuf)
        run(0, 0, 1)
        settle(cps)
        run(S1, 1, 1)
        close(1, 1, acc[rows(TILE, TILE), :], finish)

    front_scope = dict(wqkv=pltpu.VMEM((3, seq, BLK), BF16), raw=pltpu.VMEM((2, seq, BLK), F32),
                       qkv=pltpu.VMEM((3, seq, BLK), BF16), obuf=pltpu.VMEM((seq, BLK), BF16))
    def nothing():
        pass

    def tick_a():
        m0.got_ya()
        o0.take(S2)
        o0.take(S3)
        m0.take('a', S1)

    def tick_b():
        m0.relay('a', S3)
        o0.got_rx0()

    def mid_a():
        for k in SLOTS:
            o0.got_xy(k)

    def mid_b():
        m0.take('a', S2)

    def mid_c():
        m0.got_x('a', S1)
        m0.relay('b', S1)
        m0.take('b', S1)

    def tick_c():
        m0.begin_y_rest()
        q1.begin()
        for k in SLOTS:
            o0.got_r(k)
        o0.done()
        m0.relay('b', S2)

    pl.run_scoped(lambda **kw: front(0, ag_tx=None, ticks=(tick_a, tick_b, tick_c), mid_hooks=(mid_a, mid_b, mid_c), **kw), **front_scope)
    h_tx0 = []

    def proj_zero(wo):
        def wo_at(n):
            return wo.at[n]

        wo_loads(0, wo_at)
        proj(0, wo_at, wo_waits(0, wo_at), h_tx0)

    pl.run_scoped(proj_zero, pltpu.VMEM((16, BLK, BLK), BF16))

    def before_own():
        m0.relay('b', S3)
        m0.take('a', S3)
        o1.begin()
        for i in TRIO:
            m1.begin_ring(i)
        m0.got_yb()
        m0.got_x('a', S2)
        m0.got_x('b', S1)
        m1.begin_y()
        m1.begin_c()

    def before_other():
        m0.take('b', S2)
        m0.take('b', S3)
        m0.got_x('a', S3)
        for i in TRIO:
            q1.got_y(i)
        o1.relay(S1)
        o1.relay(S2)

    def before_one():
        m0.got_x('b', S2)
        m1.relay(S1, 0)
        m1.relay(S2, 0)

    def before_two():
        m0.got_x('b', S3)
        m1.take(S1, 0, spread=False)
        for i in TRIO[1:]:
            m1.relay(S2, i)

    def before_three():
        o1.relay(S3)
        m1.got_y0(0)

    def before_sum():
        for i in TRIO[1:]:
            m1.got_y0(i)
            m1.take(S1, i, spread=False)

    def after_second():
        o1.begin_y()

    ev0 = (before_own, before_one, before_two, before_three, before_sum, nothing, after_second, before_other)

    ag_marks = []
    ag = [Cast(f'ag_{t}') for t in PAIR]
    fin = [Cast(f'fin_{t}') for t in PAIR]

    def finish0(t):
        blk = rows(cz * chunk + t * TILE, TILE)
        mark = len(sent)
        ag[t].push(0, [(hb.at[rows(t * TILE, TILE), :], xbuf.at[blk, :])])
        ag_marks.append((mark, len(sent)))
        xbuf[blk, :] = hb[rows(t * TILE, TILE), :]

    pl.run_scoped(lambda wbuf, acc, msend: mlp0(wbuf, acc, msend, h_tx0, ev0, finish0),
                  pltpu.VMEM((2, 4, 3, F_HALF, BLK), BF16), pltpu.VMEM((2 * chunk, 2048), F32), pltpu.VMEM((chunk, 2048), BF16))

    def ag_block(k, t):
        return xbuf.at[rows(slot_plane(k) * chunk + t * TILE, TILE), :]

    def ag_pass(t, k):
        mark = len(sent)
        ag[t].relay(k, same([ag_block(k, t)]))
        ag_marks.append((mark, len(sent)))

    def ag_relay(k):
        for t in PAIR:
            ag_pass(t, k)

    def ag_part(k):
        if k == S2:
            ag_relay(S3)
            for i in TRIO[1:]:
                m1.relay(S1, i)
            m1.got_r0()
            o1.got_xy(S1)
            o1.got_rx0()
            for i in TRIO:
                m1.got_xy(S1, i)
        for t in PAIR:
            ag[t].take(k)
            if k == S3 and t == 0:
                o1.got_xy(S2)
                o1.got_xy(S3)
                for i in TRIO:
                    m1.got_xy(S2, i)

    def front_one(**kw):
        for t in PAIR:
            for k in (S1, S2):
                ag_pass(t, k)
        for i in TRIO:
            m1.spread(S1, i)
        for k in SLOTS:
            o1.take(k)
        for i in TRIO:
            m1.take(S2, i)
        o1.got_y0()
        for i in TRIO:
            q1.got_r(i)
        q1.done()
        front(1, ag_tx=lambda k: ag_part(k) if k else None, ticks=(tick_d, tick_e, tick_f), mid_hooks=(nothing, mid_e, nothing), **kw)

    def tick_d():
        for i in PAIR:
            m1.relay(S3, i)

    def tick_e():
        for i in TRIO:
            m1.got_r(S1, i)
        for k in SLOTS:
            o1.got_r(k)
        o1.done()
        for first, last in ag_marks:
            flush(first, last)
        wo_loads(1, wo_in_x)

    def mid_e():
        m1.take(S3, 0)

    def tick_f():
        m1.relay(S3, S2)
        for i in TRIO:
            m1.got_r(S2, i)
        m1.take(S3, S1)
        for i in PAIR:
            m1.got_xy(S3, i)

    pl.run_scoped(front_one, **front_scope)
    for first, last in ag_marks:
        flush(first, last)

    def finish1(t):
        blk = rows(cz * chunk + t * TILE, TILE)
        fin[t].push(0, [(hb.at[rows(t * TILE, TILE), :], y_ref.at[blk, :])])
        local(hb.at[rows(t * TILE, TILE), :], y_ref.at[blk, :], 1 + t)

    pl.run_scoped(lambda wbuf, acc: mlp1(wbuf, acc, finish1),
                  pltpu.VMEM((2, 4, 3, 1376, BLK), BF16), pltpu.VMEM((chunk, 2048), F32))
    def fin_block(k, t):
        return y_ref.at[rows(slot_plane(k) * chunk + t * TILE, TILE), :]

    for k in SLOTS:
        for t in PAIR:
            fin[t].relay(k, same([fin_block(k, t)]))
    flush()
    for k in SLOTS:
        for t in PAIR:
            fin[t].take(k)
    for t in PAIR:
        pltpu.make_async_copy(hb.at[rows(t * TILE, TILE), :], y_ref.at[rows(t * TILE, TILE), :], loc_sems.at[1 + t]).wait()
    flush()
    assert max(state.values()) <= N_SEM, state


def mega_call(x, wq, wk, wv, wo, wg, wu, wd, gains, tab):
    seq, width = x.shape
    any_spec = pl.BlockSpec(memory_space=pl.ANY)
    chunk = seq // 4
    outs = [jax.ShapeDtypeStruct((seq, width), BF16),
            jax.ShapeDtypeStruct((2, seq, BLK), BF16), jax.ShapeDtypeStruct((2, seq, BLK), BF16),
            jax.ShapeDtypeStruct((2, 3, 2048, BLK), BF16), jax.ShapeDtypeStruct((2, 4, 4, BLK, BLK), BF16),
            jax.ShapeDtypeStruct((4, 4, 3, F_HALF, BLK), BF16), jax.ShapeDtypeStruct((4, 4, 3, 1376, BLK), BF16)]
    return pl.pallas_call(
        mega,
        in_specs=[any_spec] * 10,
        out_specs=[any_spec] * 7,
        out_shape=outs,
        scratch_shapes=[pltpu.VMEM((seq, width), BF16), pltpu.VMEM((2 * chunk, width), BF16)] + [pltpu.VMEM((chunk, width), BF16)] + [
                        pltpu.VMEM((chunk, width), BF16), pltpu.VMEM((2, 4, 8, seq), F32),
                        pltpu.VMEM((seq, LANE), F32), pltpu.VMEM((seq, LANE), F32), pltpu.VMEM((4, 8, BLK), F32),
                        pltpu.SemaphoreType.DMA((N_SEM,)), pltpu.SemaphoreType.DMA((N_SEM,)),
                        pltpu.SemaphoreType.DMA((64,))],
        compiler_params=pltpu.CompilerParams(collective_id=0, has_side_effects=True, vmem_limit_bytes=67043328),
        name='mega')(x, wq, wk, wv, wo, wg, wu, wd, gains, tab)


def solution(mesh):
    batch_axes = ('dp', 'fsdp')
    act_spec = P(batch_axes, None, None)
    in_cols = P(None, 'fsdp', 'tp')
    in_rows = P(None, 'tp', 'fsdp')
    tp_gain = P(None, 'tp')
    fsdp_gain = P(None, 'fsdp')
    cache_spec = P(None, batch_axes, None, 'tp', None)

    def local_layers(x, w_query, w_key, w_value, w_out, w_gate, w_up, w_down, q_norm_w, k_norm_w, attn_norm_w, ffn_norm_w):
        batch, seq_len, width = x.shape
        gains = jnp.concatenate([attn_norm_w, ffn_norm_w, q_norm_w, k_norm_w], axis=0)
        tab = jnp.asarray(rope_table(seq_len))
        outs = mega_call(x.reshape(seq_len, width), w_query, w_key, w_value, w_out,
                         jnp.swapaxes(w_gate, 1, 2), jnp.swapaxes(w_up, 1, 2), w_down, gains, tab)
        shape = (2, 1, seq_len, 4, HEAD_DIM)
        return outs[0].reshape(x.shape), outs[1].reshape(shape), outs[2].reshape(shape)

    return jax.shard_map(local_layers, mesh=mesh,
                         in_specs=(act_spec, in_cols, in_cols, in_cols, in_rows, in_cols, in_cols, in_rows,
                                   tp_gain, tp_gain, fsdp_gain, fsdp_gain),
                         out_specs=(act_spec, cache_spec, cache_spec), check_vma=False)
```
